256 devices in a mesh: px: 32 (over y, z_lo, core), py: 8 (over x, z_hi).
Axes of the slice: x: 4, y: 4, z: 8 (z_hi: 2, z_lo: 4; z = z_hi * 4 + z_lo), core: 2. Of those that a mesh axis runs over, the one named last changes fastest.
Arguments:
- spectrum: float32 [2, 3, 128, 128, 512], P(None, None, 'px', 'py'), may hold values from -3 to 3
- scalar: float32 [1024, 256, 256], P('px', 'py'), may hold values from -6 to 6
Outputs:
- tendency: float32 [2, 3, 128, 128, 512], P(None, None, 'px', 'py')
- advanced: float32 [1024, 256, 256], P('px', 'py')
The draws below stay inside these ranges and needn't reach their ends.
All inputs are finite; a program needn't handle non-finite values.
Results may differ from the reference program's by a relative error of at most 0.0003.
Values sent between devices are 32-bit elements; how exact they have to be, the bound alone decides.
No kernel may reach another device: no remote copies, remote signals or barrier semaphores. Data moves between devices by JAX's collectives and lax.ppermute only.
A program may use at most 128 MiB of HBM per device.

```python
import math
import jax
import jax.numpy as jnp

V1 = 512
V2 = 128
V3 = 128
NSUB = 3


def shard_levels(own_key, extent, shards, low, top_value):
    gain = 1.0
    for dim, shards_of in shards:
        draws = jax.random.uniform(jax.random.fold_in(jax.random.fold_in(own_key, 6), dim), (shards_of,), jnp.float32, low / len(shards), top_value / len(shards))
        gain = gain * jnp.repeat(jnp.exp(draws), extent[dim] // shards_of).reshape((-1,) + (1,) * (len(extent) - 1 - dim))
    return gain


def gaussian(stream_key, shape, scale, most, split=(), held_as=jnp.bfloat16):
    drawn = jax.random.normal(stream_key, shape, jnp.float32) * scale
    if len(split) > 0:
        drawn = shard_levels(stream_key, shape, split, -0.22, 0.18) * drawn
    return jnp.clip(drawn, min=-most, max=most).astype(held_as)


def setup_inputs(seed: int = 0) -> dict:
    key_of = jax.random.split(jax.random.key(seed), 3)
    return {
        "spectrum": gaussian(key_of[0], (2, 3, V2, V3, V1), 0.5, 3.0, ((2, 32), (3, 8)), jnp.float32),
        "scalar": gaussian(key_of[1], (2 * V1, 2 * V2, 2 * V3), 1.0, 6.0, ((0, 32), (1, 8)), jnp.float32),
    }


STEP_RATIO = 0.08
DIFFUSION_RATIO = 1.0


def wavenumbers(length):
    index = jnp.arange(length, dtype=jnp.int32)
    signed = jnp.where(index < length // 2, index, index - length)
    return (2.0 * math.pi / length) * signed.astype(jnp.float32)


def upsample(field, axis):
    middles = (9.0 * (field + jnp.roll(field, -1, axis)) - (jnp.roll(field, 1, axis) + jnp.roll(field, -2, axis))) / 16.0
    paired = jnp.stack([field, middles], axis=axis + 1)
    shape = list(field.shape)
    shape[axis] = 2 * shape[axis]
    return paired.reshape(shape)


def limited_slope(first, second):
    return 0.5 * (jnp.sign(first) + jnp.sign(second)) * jnp.minimum(jnp.abs(first), jnp.abs(second))


def spin_divergence(theta, speed, axis):
    ahead = jnp.roll(theta, -1, axis)
    jump = ahead - theta
    slope = limited_slope(jnp.roll(jump, 1, axis), jump)
    left = theta + 0.5 * slope
    right = ahead - 0.5 * jnp.roll(slope, -1, axis)
    face = 0.5 * (speed + jnp.roll(speed, -1, axis))
    flux = jnp.maximum(face, 0.0) * left + jnp.minimum(face, 0.0) * right - DIFFUSION_RATIO * jump
    return flux - jnp.roll(flux, 1, axis)


def reference(spectrum, scalar):
    coeffs = jnp.transpose(spectrum[0] + 1j * spectrum[1], (0, 3, 1, 2))
    wave_first = wavenumbers(V1)[:, None, None]
    wave_second = wavenumbers(V2)[None, :, None]
    wave_third = wavenumbers(V3)[None, None, :]
    cross = jnp.stack([wave_second * coeffs[2] - wave_third * coeffs[1],
                       wave_third * coeffs[0] - wave_first * coeffs[2],
                       wave_first * coeffs[1] - wave_second * coeffs[0]])
    fields = jnp.concatenate([coeffs, 1j * cross])
    physical = jnp.real(jnp.fft.ifftn(fields, axes=(1, 2, 3), norm="ortho"))
    velocity = physical[:3]
    vorticity = physical[3:]
    speed = velocity
    for axis in (3, 1, 2):
        speed = upsample(speed, axis)
    theta = scalar
    for turn in range(NSUB):
        total = spin_divergence(theta, speed[0], 0) + spin_divergence(theta, speed[1], 1) + spin_divergence(theta, speed[2], 2)
        theta = theta - STEP_RATIO * total
    buoyancy = theta.reshape(V1, 2, V2, 2, V3, 2).mean(axis=(1, 3, 5))
    forcing = jnp.stack([velocity[1] * vorticity[2] - velocity[2] * vorticity[1],
                         velocity[2] * vorticity[0] - velocity[0] * vorticity[2],
                         velocity[0] * vorticity[1] - velocity[1] * vorticity[0] + buoyancy])
    spectral = jnp.transpose(jnp.fft.fftn(forcing, axes=(1, 2, 3), norm="ortho"), (0, 2, 3, 1))
    tendency = jnp.stack([jnp.real(spectral), jnp.imag(spectral)])
    return tendency, theta
```

```python
import math

import jax
import jax.numpy as jnp
import numpy as np
from jax import lax
from jax.experimental import pallas as pl
from jax.experimental.pallas import tpu as pltpu
from jax.sharding import PartitionSpec as P

NSUB = 3
STEP_RATIO = 0.08
DIFFUSION_RATIO = 1.0
INTERPRET = False

N1, N2, N3 = 512, 128, 128
GX, GY = 32, 8
Q2, Q3 = N2 // GX, N3 // GY
C1, C2 = N1 // GX, N2 // GY
FACTOR = 1.0 / math.sqrt(N1 * N2 * N3)
BF = jnp.bfloat16
F32 = jnp.float32


def halves(table):
    high = table.astype(np.float32).astype(BF)
    low = (table - high.astype(np.float64)).astype(np.float32).astype(BF)
    return np.asarray(high), np.asarray(low)


def waves_np(n):
    index = np.arange(n)
    return 2.0 * math.pi / n * np.where(index < n // 2, index, index - n)


def angles(n):
    index = np.arange(n)
    return 2.0 * math.pi / n * (np.outer(index, index) % n)


def first_table():
    a = angles(N1)
    return halves(np.concatenate([np.cos(a), np.sin(a)], axis=1))


def second_forward():
    a = angles(N2)
    plain = np.zeros((2, N2, N2, 2))
    plain[0, :, :, 0] = np.cos(a)
    plain[0, :, :, 1] = -np.sin(a)
    plain[1, :, :, 0] = np.sin(a)
    plain[1, :, :, 1] = np.cos(a)
    turned = np.zeros_like(plain)
    turned[0] = -plain[1]
    turned[1] = plain[0]
    both = np.stack([plain, turned]).reshape(2, 2 * N2, 2 * N2)
    return halves(both)


def third_forward():
    a = angles(N3)
    return halves(FACTOR * np.concatenate([np.cos(a), -np.sin(a)], axis=0))


def third_back():
    a = angles(N3)
    return halves(FACTOR * np.concatenate([np.cos(a), -np.sin(a)], axis=1))


def second_back():
    a = angles(N2)
    table = np.zeros((N2, 2, 2, N2))
    table[:, 0, 0] = np.cos(a)
    table[:, 0, 1] = np.sin(a)
    table[:, 1, 0] = -np.sin(a)
    table[:, 1, 1] = np.cos(a)
    return halves(table.reshape(2 * N2, 2 * N2))


def split(x):
    high = x.astype(BF)
    return high, (x - high.astype(F32)).astype(BF)


def dots(pairs, dims):
    total = None
    for left, right in pairs:
        part = lax.dot_general(left, right, (dims, ((), ())), preferred_element_type=F32)
        total = part if total is None else total + part
    return total


def dot3(left, right, dims=((1,), (0,))):
    lh, ll = left
    rh, rl = right
    return dots([(lh, rl), (ll, rh), (lh, rh)], dims)


def swap_groups(v):
    lane = lax.broadcasted_iota(jnp.int32, v[0].shape, len(v[0].shape) - 1) // 16
    axis = len(v[0].shape) - 1
    v = list(v)
    for s in (1, 2, 4):
        upper = (lane // s) % 2 == 1
        for i in range(8):
            if i & s:
                continue
            a, b = v[i], v[i + s]
            v[i] = jnp.where(upper, pltpu.roll(b, 16 * s, axis), a)
            v[i + s] = jnp.where(upper, b, pltpu.roll(a, 128 - 16 * s, axis))
    return v


def first_kernel(spec, wave, th, tl, out, y):
    rows = []
    for f in (0, 1, 2, 1, 2):
        plain, turned = [], []
        for r in range(Q2):
            re, im = spec[0, f, r], spec[1, f, r]
            plain += [re, im]
            turned += [-im, re]
        piece = jnp.concatenate(
            [jnp.concatenate(plain, axis=0), jnp.concatenate(turned, axis=0)], axis=1
        )
        rows.append(piece if len(rows) < 3 else piece * wave[...])
    table = (th[...], tl[...])
    z = dot3(table, split(jnp.concatenate(rows, axis=0)), ((1,), (1,)))
    for f in range(5):
        y[N1 * f : N1 * f + N1, :] = z[:, 128 * f : 128 * f + 128]
    for f in range(5):
        w = swap_groups([y[pl.ds(N1 * f + i, N1 // 8, stride=8), :] for i in range(8)])
        for g in range(8):
            y[pl.ds(N1 * f + g, N1 // 8, stride=8), :] = w[g]
        out[:, 16 * f : 16 * f + 16, :] = y[N1 * f : N1 * f + N1, :].reshape(GX, 16, 128)


def second_kernel(got, wave2, wave3, th, tl, out):
    c = []
    for f in range(5):
        halves_ = [got[:, 16 * f + 8 * h : 16 * f + 8 * h + 8, :].reshape(256, 128) for h in range(2)]
        c.append(jnp.concatenate(halves_, axis=1))
    k2 = wave2[...]
    k3 = wave3[...]
    curl = [k2 * c[2] - k3 * c[1], k3 * c[0] - c[4], c[3] - k2 * c[0]]
    z = []
    for group, fields in enumerate((c[:3], curl)):
        data = split(jnp.concatenate(fields, axis=1))
        z.append(dot3((th[group], tl[group]), data))
    for f in range(6):
        for ri in range(2):
            for h in range(2):
                at = ((f * 2 + ri) * 2 + h) * 16
                col = (f % 3) * 256 + h * 128
                piece = z[f // 3][ri * 128 : ri * 128 + 128, col : col + 128]
                out[:, at : at + 16, :] = piece.reshape(GY, 16, 128)


def third_kernel(got, th, tl, velocity, vorticity):
    for f in range(6):
        lines = []
        for ri in range(2):
            blocks = []
            for h in range(2):
                at = ((f * 2 + ri) * 2 + h) * 16
                blocks += swap_groups([got[q, at : at + 16, :] for q in range(GY)])
            lines.append(jnp.concatenate(blocks, axis=0))
        u = dot3(split(jnp.concatenate(lines, axis=1)), (th[...], tl[...]))
        out = velocity if f < 3 else vorticity
        out[f % 3] = u.reshape(C1, C2, N3)


def force_kernel(velocity, vorticity, buoyancy, th, tl, out):
    u = [velocity[i].reshape(C1 * C2, N3) for i in range(3)]
    w = [vorticity[i].reshape(C1 * C2, N3) for i in range(3)]
    b = buoyancy[...].reshape(C1 * C2, N3)
    force = [u[1] * w[2] - u[2] * w[1], u[2] * w[0] - u[0] * w[2], u[0] * w[1] - u[1] * w[0] + b]
    for f in range(3):
        lines = dot3(split(force[f]), (th[...], tl[...]))
        for ri in range(2):
            for h in range(2):
                at = ((f * 2 + ri) * 2 + h) * 16
                v = [
                    lines[(h * 8 + i) * 16 : (h * 8 + i) * 16 + 16, ri * 128 : ri * 128 + 128]
                    for i in range(8)
                ]
                w8 = swap_groups(v)
                for q in range(GY):
                    out[q, at : at + 16, :] = w8[q]


def second_back_kernel(got, th, tl, out):
    columns = []
    for f in range(3):
        for h in range(2):
            parts = []
            for ri in range(2):
                at = ((f * 2 + ri) * 2 + h) * 16
                parts.append(got[:, at : at + 16, :].reshape(128, 128))
            columns.append(jnp.concatenate(parts, axis=0))
    z = dot3((th[...], tl[...]), split(jnp.concatenate(columns, axis=1)))
    for f in range(3):
        for h in range(2):
            at = f * 16 + h * 8
            col = (f * 2 + h) * 128
            out[:, at : at + 8, :] = z[:, col : col + 128].reshape(GX, 8, 128)


def first_back_kernel(got, th, tl, out, y):
    rows = []
    for f in range(3):
        y[...] = got[:, 16 * f : 16 * f + 16, :].reshape(N1, 128)
        w = swap_groups([y[pl.ds(g, N1 // 8, stride=8), :] for g in range(8)])
        for i in range(8):
            y[pl.ds(i, N1 // 8, stride=8), :] = w[i]
        rows.append(y[...].T)
    z = dot3(split(jnp.concatenate(rows, axis=0)), (th[...], tl[...]))
    for f in range(3):
        for r in range(Q2):
            at = f * 128 + r * 32
            cr, ci = z[at : at + 16, :N1], z[at + 16 : at + 32, :N1]
            sr, si = z[at : at + 16, N1:], z[at + 16 : at + 32, N1:]
            out[0, f, r] = cr + si
            out[1, f, r] = ci - sr


def call(kernel, out_shape, *args, scratch=()):
    return pl.pallas_call(
        kernel,
        out_shape=out_shape,
        scratch_shapes=list(scratch),
        interpret=INTERPRET,
        name=kernel.__name__,
        compiler_params=pltpu.CompilerParams(vmem_limit_bytes=48 * 1024 * 1024),
    )(*args)


def shape(*dims):
    return jax.ShapeDtypeStruct(dims, F32)


def padded(block, sides, width):
    for axis, dim in sides:
        count = lax.axis_size(axis)
        forward = [(i, i + 1) for i in range(count - 1)]
        forward.append((count - 1, 0))
        backward = [(target, source) for source, target in forward]
        low = lax.ppermute(
            lax.slice_in_dim(block, block.shape[dim] - width, None, axis=dim), axis, forward
        )
        high = lax.ppermute(lax.slice_in_dim(block, 0, width, axis=dim), axis, backward)
        block = jnp.concatenate([low, block, high], axis=dim)
    return block


def padded_2(shard, sides, width):
    edges = {}
    for axis, dim in sides:
        peers, length = (lax.axis_size(axis), shard.shape[dim])
        up = [(i, (i + 1) % peers) for i in range(peers)]
        last = lax.slice_in_dim(shard, length - width, length, axis=dim)
        first = lax.slice_in_dim(shard, 0, width, axis=dim)
        edges[dim] = (
            lax.ppermute(last, axis, up),
            lax.ppermute(first, axis, [(b, a) for a, b in up]),
        )
    done = []
    for _, dim in sides:
        low, high = edges[dim]
        around = [(width, width) if d in done else (0, 0) for d in range(shard.ndim)]
        shard = jnp.concatenate([jnp.pad(low, around), shard, jnp.pad(high, around)], axis=dim)
        done.append(dim)
    return shard


def contract(form, left, right):
    return jnp.einsum(form, left, right, precision=lax.Precision.HIGHEST)


def upsample_table(length):
    rows = jnp.arange(length, dtype=jnp.int32)[:, None]
    cols = jnp.arange(2 * length, dtype=jnp.int32)[None, :]
    half = cols // 2
    is_odd = cols % 2 == 1
    near = jnp.logical_or(rows == half, rows == (half + 1) % length)
    distant = jnp.logical_or(rows == (half - 1) % length, rows == (half + 2) % length)
    even_part = jnp.where(jnp.logical_and(jnp.logical_not(is_odd), rows == half), 1.0, 0.0)
    odd_part = jnp.where(
        is_odd, jnp.where(near, 9.0 / 16.0, 0.0) - jnp.where(distant, 1.0 / 16.0, 0.0), 0.0
    )
    return (even_part + odd_part).astype(jnp.float32)


def pair_table(length):
    rows = jnp.arange(2 * length, dtype=jnp.int32)[:, None]
    cols = jnp.arange(length, dtype=jnp.int32)[None, :]
    return jnp.where(rows // 2 == cols, 0.125, 0.0).astype(jnp.float32)


def slab(array, start, stop, axis):
    return lax.slice_in_dim(array, start, stop, axis=axis)


def refine(field, axis):
    count = field.shape[axis]
    points = slab(field, 2, count - 1, axis)
    middles = (
        9.0 * (slab(field, 1, count - 2, axis) + points)
        - (slab(field, 0, count - 3, axis) + slab(field, 3, count, axis))
    ) / 16.0
    paired = jnp.concatenate([middles, points], axis=axis + 1)
    shape = list(field.shape)
    shape[axis] = 2 * (count - 3)
    return paired.reshape(shape)


def limited_slope(first, second):
    return 0.5 * (jnp.sign(first) + jnp.sign(second)) * jnp.minimum(jnp.abs(first), jnp.abs(second))


def spin_divergence(theta, speed, axis):
    ahead = jnp.roll(theta, -1, axis)
    jump = ahead - theta
    slope = limited_slope(jnp.roll(jump, 1, axis), jump)
    left = theta + 0.5 * slope
    right = ahead - 0.5 * jnp.roll(slope, -1, axis)
    face = 0.5 * (speed + jnp.roll(speed, -1, axis))
    flux = jnp.maximum(face, 0.0) * left + jnp.minimum(face, 0.0) * right - DIFFUSION_RATIO * jump
    return flux - jnp.roll(flux, 1, axis)


def divergence(theta, speed, axis):
    count = theta.shape[axis]
    jump = slab(theta, 1, count, axis) - slab(theta, 0, count - 1, axis)
    slope = limited_slope(slab(jump, 0, count - 2, axis), slab(jump, 1, count - 1, axis))
    left = slab(theta, 1, count - 2, axis) + 0.5 * slab(slope, 0, count - 3, axis)
    right = slab(theta, 2, count - 1, axis) - 0.5 * slab(slope, 1, count - 2, axis)
    face = 0.5 * (slab(speed, 0, count - 3, axis) + slab(speed, 1, count - 2, axis))
    flux = (
        jnp.maximum(face, 0.0) * left
        + jnp.minimum(face, 0.0) * right
        - DIFFUSION_RATIO * slab(jump, 1, count - 2, axis)
    )
    return slab(flux, 1, count - 3, axis) - slab(flux, 0, count - 4, axis)


def advance(theta, speed):
    flow_first = divergence(theta[:, 1:-1], speed[0], 0)[:, 1:-1]
    flow_second = divergence(theta[1:-1, :], speed[1], 1)[1:-1, :]
    flow_third = spin_divergence(theta[1:-1, 1:-1], speed[2], 2)[1:-1, 1:-1]
    return theta[2:-2, 2:-2] - STEP_RATIO * (flow_first + flow_second + flow_third)


def body(spectrum, scalar):
    wave_first = np.tile(waves_np(N1).astype(np.float32), 2)[None]
    wave_second = np.repeat(waves_np(N2).astype(np.float32), 2)[:, None]
    blocks = np.tile(waves_np(N3).astype(np.float32).reshape(GY, 1, Q3), (1, 16, 1)).reshape(GY, 1, 256)
    wave_third = lax.dynamic_index_in_dim(jnp.asarray(blocks), lax.axis_index("py"), 0, keepdims=False)
    first = [jnp.asarray(t) for t in first_table()]
    second = [jnp.asarray(t) for t in second_forward()]
    third = [jnp.asarray(t) for t in third_forward()]
    sent = call(
        first_kernel, shape(GX, 80, 128), spectrum, jnp.asarray(wave_first), *first,
        scratch=(pltpu.VMEM((5 * N1, 128), F32),),
    )
    got = lax.all_to_all(sent, "px", split_axis=0, concat_axis=0, tiled=True)
    sent = call(second_kernel, shape(GY, 384, 128), got, jnp.asarray(wave_second), wave_third, *second)
    got = lax.all_to_all(sent, "py", split_axis=0, concat_axis=0, tiled=True)
    velocity, vorticity = call(
        third_kernel, (shape(3, C1, C2, N3), shape(3, C1, C2, N3)), got, *third
    )
    widened = padded(velocity, (("px", 1), ("py", 2)), 4)
    speed = contract("cxyz,zw->cxyw", widened, upsample_table(N3))
    speed = refine(speed, 1)
    speed = refine(speed, 2)
    theta = scalar
    inner_speed = speed[:, 4:-4, 4:-4]
    for turn in range(NSUB):
        grown = padded_2(theta, (("px", 0), ("py", 1)), 2)
        theta = advance(grown, inner_speed)
    pair_first = theta.reshape(C1, 2, 2 * C2, 2 * N3).sum(axis=1)
    pair_both = pair_first.reshape(C1, C2, 4 * N3)
    pair_both = pair_both[..., : 2 * N3] + pair_both[..., 2 * N3 :]
    buoyancy = contract("xyw,wz->xyz", pair_both, pair_table(N3))
    sent = call(
        force_kernel, shape(GY, 192, 128), velocity, vorticity, buoyancy,
        *[jnp.asarray(t) for t in third_back()],
    )
    got = lax.all_to_all(sent, "py", split_axis=0, concat_axis=0, tiled=True)
    sent = call(
        second_back_kernel, shape(GX, 48, 128), got, *[jnp.asarray(t) for t in second_back()]
    )
    got = lax.all_to_all(sent, "px", split_axis=0, concat_axis=0, tiled=True)
    tendency = call(
        first_back_kernel, shape(2, 3, Q2, Q3, N1), got, *first,
        scratch=(pltpu.VMEM((N1, 128), F32),),
    )
    return tendency, theta


def solution(mesh):
    in_specs = (P(None, None, "px", "py", None), P("px", "py", None))
    out_specs = (P(None, None, "px", "py", None), P("px", "py", None))
    return jax.shard_map(body, mesh=mesh, in_specs=in_specs, out_specs=out_specs, check_vma=False)
```

```python
import math

import jax
import jax.numpy as jnp
import numpy as np
from jax import lax
from jax.experimental import pallas as pl
from jax.experimental.pallas import tpu as pltpu
from jax.sharding import PartitionSpec as P

NSUB = 3
STEP_RATIO = 0.08
DIFFUSION_RATIO = 1.0
INTERPRET = False

N1, N2, N3 = 512, 128, 128
GX, GY = 32, 8
Q2, Q3 = N2 // GX, N3 // GY
C1, C2 = N1 // GX, N2 // GY
FACTOR = 1.0 / math.sqrt(N1 * N2 * N3)
BF = jnp.bfloat16
F32 = jnp.float32


def halves(table):
    high = table.astype(np.float32).astype(BF)
    low = (table - high.astype(np.float64)).astype(np.float32).astype(BF)
    return np.asarray(high), np.asarray(low)


def waves_np(n):
    index = np.arange(n)
    return 2.0 * math.pi / n * np.where(index < n // 2, index, index - n)


def angles(n):
    index = np.arange(n)
    return 2.0 * math.pi / n * (np.outer(index, index) % n)


def first_table():
    a = angles(N1)
    return halves(np.concatenate([np.cos(a), np.sin(a)], axis=1))


def second_forward():
    a = angles(N2)
    plain = np.zeros((2, N2, N2, 2))
    plain[0, :, :, 0] = np.cos(a)
    plain[0, :, :, 1] = -np.sin(a)
    plain[1, :, :, 0] = np.sin(a)
    plain[1, :, :, 1] = np.cos(a)
    turned = np.zeros_like(plain)
    turned[0] = -plain[1]
    turned[1] = plain[0]
    both = np.stack([plain, turned]).reshape(2, 2 * N2, 2 * N2)
    return halves(both)


def third_forward():
    a = angles(N3)
    return halves(FACTOR * np.concatenate([np.cos(a), -np.sin(a)], axis=0))


def third_back():
    a = angles(N3)
    return halves(FACTOR * np.concatenate([np.cos(a), -np.sin(a)], axis=1))


def second_back():
    a = angles(N2)
    table = np.zeros((N2, 2, 2, N2))
    table[:, 0, 0] = np.cos(a)
    table[:, 0, 1] = np.sin(a)
    table[:, 1, 0] = -np.sin(a)
    table[:, 1, 1] = np.cos(a)
    return halves(table.reshape(2 * N2, 2 * N2))


def split(x):
    high = x.astype(BF)
    return high, (x - high.astype(F32)).astype(BF)


def dots(pairs, dims):
    total = None
    for left, right in pairs:
        part = lax.dot_general(left, right, (dims, ((), ())), preferred_element_type=F32)
        total = part if total is None else total + part
    return total


def dot3(left, right, dims=((1,), (0,))):
    lh, ll = left
    rh, rl = right
    return dots([(lh, rl), (ll, rh), (lh, rh)], dims)


def swap_groups(v):
    lane = lax.broadcasted_iota(jnp.int32, v[0].shape, len(v[0].shape) - 1) // 16
    axis = len(v[0].shape) - 1
    v = list(v)
    for s in (1, 2, 4):
        upper = (lane // s) % 2 == 1
        for i in range(8):
            if i & s:
                continue
            a, b = v[i], v[i + s]
            v[i] = jnp.where(upper, pltpu.roll(b, 16 * s, axis), a)
            v[i + s] = jnp.where(upper, b, pltpu.roll(a, 128 - 16 * s, axis))
    return v


def first_kernel(spec, wave, th, tl, out, y):
    rows = []
    for f in (0, 1, 2, 1, 2):
        plain, turned = [], []
        for r in range(Q2):
            re, im = spec[0, f, r], spec[1, f, r]
            plain += [re, im]
            turned += [-im, re]
        piece = jnp.concatenate(
            [jnp.concatenate(plain, axis=0), jnp.concatenate(turned, axis=0)], axis=1
        )
        rows.append(piece if len(rows) < 3 else piece * wave[...])
    table = (th[...], tl[...])
    z = dot3(table, split(jnp.concatenate(rows, axis=0)), ((1,), (1,)))
    for f in range(5):
        y[N1 * f : N1 * f + N1, :] = z[:, 128 * f : 128 * f + 128]
    for f in range(5):
        w = swap_groups([y[pl.ds(N1 * f + i, N1 // 8, stride=8), :] for i in range(8)])
        for g in range(8):
            y[pl.ds(N1 * f + g, N1 // 8, stride=8), :] = w[g]
        out[:, 16 * f : 16 * f + 16, :] = y[N1 * f : N1 * f + N1, :].reshape(GX, 16, 128)


def second_kernel(got, wave2, wave3, th, tl, out):
    c = []
    for f in range(5):
        halves_ = [got[:, 16 * f + 8 * h : 16 * f + 8 * h + 8, :].reshape(256, 128) for h in range(2)]
        c.append(jnp.concatenate(halves_, axis=1))
    k2 = wave2[...]
    k3 = wave3[...]
    curl = [k2 * c[2] - k3 * c[1], k3 * c[0] - c[4], c[3] - k2 * c[0]]
    z = []
    for group, fields in enumerate((c[:3], curl)):
        data = split(jnp.concatenate(fields, axis=1))
        z.append(dot3((th[group], tl[group]), data))
    for f in range(6):
        for ri in range(2):
            for h in range(2):
                at = ((f * 2 + ri) * 2 + h) * 16
                col = (f % 3) * 256 + h * 128
                piece = z[f // 3][ri * 128 : ri * 128 + 128, col : col + 128]
                out[:, at : at + 16, :] = piece.reshape(GY, 16, 128)


def third_kernel(got, th, tl, velocity, vorticity):
    for f in range(6):
        lines = []
        for ri in range(2):
            blocks = []
            for h in range(2):
                at = ((f * 2 + ri) * 2 + h) * 16
                blocks += swap_groups([got[q, at : at + 16, :] for q in range(GY)])
            lines.append(jnp.concatenate(blocks, axis=0))
        u = dot3(split(jnp.concatenate(lines, axis=1)), (th[...], tl[...]))
        out = velocity if f < 3 else vorticity
        out[f % 3] = u.reshape(C1, C2, N3)


def force_lines(velocity, vorticity, b, th, tl, out):
    u = [velocity[i].reshape(C1 * C2, N3) for i in range(3)]
    w = [vorticity[i].reshape(C1 * C2, N3) for i in range(3)]
    force = [u[1] * w[2] - u[2] * w[1], u[2] * w[0] - u[0] * w[2], u[0] * w[1] - u[1] * w[0] + b]
    for f in range(3):
        lines = dot3(split(force[f]), (th[...], tl[...]))
        for ri in range(2):
            for h in range(2):
                at = ((f * 2 + ri) * 2 + h) * 16
                v = [
                    lines[(h * 8 + i) * 16 : (h * 8 + i) * 16 + 16, ri * 128 : ri * 128 + 128]
                    for i in range(8)
                ]
                w8 = swap_groups(v)
                for q in range(GY):
                    out[q, at : at + 16, :] = w8[q]


def rise_tables():
    plain = np.zeros((N3, 2 * N3))
    for i in range(N3):
        plain[i, 2 * i] += 1.0
        for near in (i, (i + 1) % N3):
            plain[near, 2 * i + 1] += 9.0 / 16.0
        for far in ((i - 1) % N3, (i + 2) % N3):
            plain[far, 2 * i + 1] -= 1.0 / 16.0
    face = 0.5 * (plain + np.roll(plain, -1, axis=1))
    return np.stack([plain, face]).astype(np.float32).astype(BF)


def pair_table():
    cols = np.arange(2 * N3)[:, None] // 2
    return np.where(cols == np.arange(N3)[None], 0.125, 0.0).astype(np.float32).astype(BF)


def middle(a, b, c, d):
    return (9.0 * (b + c) - (a + d)) * (1.0 / 16.0)


def limited(first, second):
    return jnp.maximum(jnp.minimum(second, 0.0), jnp.minimum(first, jnp.maximum(second, 0.0)))


def upwind(face, left, right, jump):
    return face * jnp.where(face > 0.0, left, right) - DIFFUSION_RATIO * jump


def rolled_divergence(theta, face, axis):
    count = theta.shape[axis]
    jump = pltpu.roll(theta, count - 1, axis) - theta
    half = 0.5 * limited(pltpu.roll(jump, 1, axis), jump)
    flux = upwind(face, theta + half, pltpu.roll(theta - half, count - 1, axis), jump)
    return flux - pltpu.roll(flux, 1, axis)


EDGE = 6
SLABS = 2 * C1 + 2 * EDGE
ROWS = 2 * C2 + 16
PTS = C1 + 8
PROWS = C2 + 16


def scalar_kernel(
    scalar, x_low, x_high, y_low, y_high,
    velocity, vx_low, vx_high, vy_low, vy_high, vorticity,
    rise, pair, th, tl,
    advanced, out,
    ta, tb, vw, su, sf, f1, f2, f3, bs,
):
    for c in range(3):
        vw[c * PTS : c * PTS + 4, 8:24, :] = vx_low[c]
        vw[c * PTS + 4 : c * PTS + 20, 8:24, :] = velocity[c]
        vw[c * PTS + 20 : c * PTS + 24, 8:24, :] = vx_high[c]
        vw[c * PTS : c * PTS + 24, 4:8, :] = vy_low[c]
        vw[c * PTS : c * PTS + 24, 24:28, :] = vy_high[c]
    total = 3 * PTS * PROWS
    for c in range(3):
        table = rise[1 if c == 2 else 0]

        def third(n, carry, c=c, table=table):
            lines = vw[pl.ds(c * PTS + 8 * n, 8)].reshape(8 * PROWS, N3)
            high, low = split(lines)
            z = dots([(low, table), (high, table)], ((1,), (0,)))
            at = pl.multiple_of((c * PTS + 8 * n) * PROWS, 8)
            for h in range(2):
                su[pl.ds(h * total + at, 8 * PROWS), :] = z[:, h * 128 : h * 128 + 128]
            return carry

        lax.fori_loop(0, PTS // 8, third, 0)

    def second(n, carry, c):
        for h in range(2):
            at = pl.multiple_of(h * total + (c * PTS + n) * PROWS, 8)
            p = su[pl.ds(at, PROWS), :]
            a, b, cc, d = (p[4 + o : 25 + o] for o in range(4))
            odd, even = middle(a, b, cc, d), cc
            to = (h * 3 * PTS + c * PTS + n) * ROWS
            if c == 1:
                sf[pl.ds(to + 3, 21, stride=2), :] = 0.5 * (odd + even)
                sf[pl.ds(to + 2, 21, stride=2), :] = 0.5 * (b + odd)
            else:
                sf[pl.ds(to + 3, 21, stride=2), :] = odd
                sf[pl.ds(to + 4, 21, stride=2), :] = even
        return carry

    for c in range(3):
        lax.fori_loop(0, PTS, lambda n, k, c=c: second(n, k, c), 0)

    def first(k, carry):
        for c, face in enumerate((f1, f2, f3)):
            for h in range(2):
                cols = pl.ds(h * 128, 128)
                a, b, cc, d = (
                    sf[pl.ds(pl.multiple_of((h * 3 * PTS + c * PTS + k + o) * ROWS, 8), ROWS), :]
                    for o in range(4)
                )
                odd = middle(a, b, cc, d)
                if c == 0:
                    face[2 * k + 1, :, cols] = 0.5 * (odd + cc)
                    face[2 * k, :, cols] = 0.5 * (b + odd)
                else:
                    face[2 * k + 1, :, cols] = odd
                    face[2 * k + 2, :, cols] = cc
        return carry

    lax.fori_loop(0, 21, first, 0)

    ta[0:EDGE, 8:40, :] = x_low[...]
    ta[EDGE : EDGE + 2 * C1, 8:40, :] = scalar[...]
    ta[EDGE + 2 * C1 :, 8:40, :] = x_high[...]
    ta[:, 0:8, :] = y_low[...]
    ta[:, 40:48, :] = y_high[...]

    for turn, (source, target) in enumerate(((ta, tb), (tb, ta), (ta, tb))):
        low = 2 + 2 * turn
        t0, t1, t2, t3 = (source[low - 2 + o] for o in range(4))
        j0, j1, j2 = t1 - t0, t2 - t1, t3 - t2
        h1, h2 = 0.5 * limited(j0, j1), 0.5 * limited(j1, j2)
        flux = upwind(f1[low - 1], t1 + h1, t2 - h2, j1)

        def step(i, carry, source=source, target=target, turn=turn):
            left, jump, before = carry
            here, ahead = source[i], source[i + 1]
            next_jump = source[i + 2] - ahead
            half = 0.5 * limited(jump, next_jump)
            flux = upwind(f1[i], left, ahead - half, jump)
            change = flux - before
            change += rolled_divergence(here, f2[i], 0)
            change += rolled_divergence(here, f3[i], 1)
            fresh = here - STEP_RATIO * change
            if turn < NSUB - 1:
                target[i] = fresh
            else:
                advanced[i - EDGE] = fresh[8:40]
            return ahead + half, next_jump, flux

        lax.fori_loop(low, SLABS - low, step, (t2 + h2, j2, flux))

    def pairs(n, carry):
        lines = (advanced[pl.ds(4 * n, 4)]).reshape(2, 2, 32, 256)
        both = (lines[:, 0] + lines[:, 1]).reshape(64, 256)
        high, low = split(both)
        bs[pl.ds(pl.multiple_of(64 * n, 8), 64), :] = dots([(low, pair[...]), (high, pair[...])], ((1,), (0,)))
        return carry

    lax.fori_loop(0, C1 // 2, pairs, 0)
    buoyancy = bs[pl.ds(0, C1 * C2, stride=2), :] + bs[pl.ds(1, C1 * C2, stride=2), :]
    force_lines(velocity, vorticity, buoyancy, th, tl, out)


def second_back_kernel(got, th, tl, out):
    columns = []
    for f in range(3):
        for h in range(2):
            parts = []
            for ri in range(2):
                at = ((f * 2 + ri) * 2 + h) * 16
                parts.append(got[:, at : at + 16, :].reshape(128, 128))
            columns.append(jnp.concatenate(parts, axis=0))
    z = dot3((th[...], tl[...]), split(jnp.concatenate(columns, axis=1)))
    for f in range(3):
        for h in range(2):
            at = f * 16 + h * 8
            col = (f * 2 + h) * 128
            out[:, at : at + 8, :] = z[:, col : col + 128].reshape(GX, 8, 128)


def first_back_kernel(got, th, tl, out, y):
    rows = []
    for f in range(3):
        y[...] = got[:, 16 * f : 16 * f + 16, :].reshape(N1, 128)
        w = swap_groups([y[pl.ds(g, N1 // 8, stride=8), :] for g in range(8)])
        for i in range(8):
            y[pl.ds(i, N1 // 8, stride=8), :] = w[i]
        rows.append(y[...].T)
    z = dot3(split(jnp.concatenate(rows, axis=0)), (th[...], tl[...]))
    for f in range(3):
        for r in range(Q2):
            at = f * 128 + r * 32
            cr, ci = z[at : at + 16, :N1], z[at + 16 : at + 32, :N1]
            sr, si = z[at : at + 16, N1:], z[at + 16 : at + 32, N1:]
            out[0, f, r] = cr + si
            out[1, f, r] = ci - sr


def call(kernel, out_shape, *args, scratch=()):
    return pl.pallas_call(
        kernel,
        out_shape=out_shape,
        scratch_shapes=list(scratch),
        interpret=INTERPRET,
        name=kernel.__name__,
        compiler_params=pltpu.CompilerParams(vmem_limit_bytes=48 * 1024 * 1024),
    )(*args)


def shape(*dims):
    return jax.ShapeDtypeStruct(dims, F32)


def ring(axis):
    count = lax.axis_size(axis)
    up = [(i, (i + 1) % count) for i in range(count)]
    return up, [(b, a) for a, b in up]


def edges(axis, first, last):
    up, down = ring(axis)
    return lax.ppermute(last, axis, up), lax.ppermute(first, axis, down)


def body(spectrum, scalar):
    wave_first = np.tile(waves_np(N1).astype(np.float32), 2)[None]
    wave_second = np.repeat(waves_np(N2).astype(np.float32), 2)[:, None]
    blocks = np.tile(waves_np(N3).astype(np.float32).reshape(GY, 1, Q3), (1, 16, 1)).reshape(GY, 1, 256)
    wave_third = lax.dynamic_index_in_dim(jnp.asarray(blocks), lax.axis_index("py"), 0, keepdims=False)
    first = [jnp.asarray(t) for t in first_table()]
    second = [jnp.asarray(t) for t in second_forward()]
    third = [jnp.asarray(t) for t in third_forward()]
    x_low, x_high = edges("px", scalar[:EDGE], scalar[-EDGE:])
    strips = [
        jnp.concatenate([part[:, cut] for part in (x_low, scalar, x_high)], axis=0)
        for cut in (slice(0, 8), slice(2 * C2 - 8, 2 * C2))
    ]
    y_low, y_high = edges("py", *strips)
    sent = call(
        first_kernel, shape(GX, 80, 128), spectrum, jnp.asarray(wave_first), *first,
        scratch=(pltpu.VMEM((5 * N1, 128), F32),),
    )
    got = lax.all_to_all(sent, "px", split_axis=0, concat_axis=0, tiled=True)
    sent = call(second_kernel, shape(GY, 384, 128), got, jnp.asarray(wave_second), wave_third, *second)
    got = lax.all_to_all(sent, "py", split_axis=0, concat_axis=0, tiled=True)
    velocity, vorticity = call(
        third_kernel, (shape(3, C1, C2, N3), shape(3, C1, C2, N3)), got, *third
    )
    vx_low, vx_high = edges("px", velocity[:, :4], velocity[:, -4:])
    strips = [
        jnp.concatenate([part[:, :, cut] for part in (vx_low, velocity, vx_high)], axis=1)
        for cut in (slice(0, 4), slice(C2 - 4, C2))
    ]
    vy_low, vy_high = edges("py", *strips)
    theta, sent = call(
        scalar_kernel, (shape(2 * C1, 2 * C2, 2 * N3), shape(GY, 192, 128)),
        scalar, x_low, x_high, y_low, y_high,
        velocity, vx_low, vx_high, vy_low, vy_high, vorticity,
        jnp.asarray(rise_tables()), jnp.asarray(pair_table()), *[jnp.asarray(t) for t in third_back()],
        scratch=(
            pltpu.VMEM((SLABS, ROWS, 256), F32),
            pltpu.VMEM((SLABS, ROWS, 256), F32),
            pltpu.VMEM((3 * PTS, PROWS, N3), F32),
            pltpu.VMEM((2 * 3 * PTS * PROWS, 128), F32),
            pltpu.VMEM((2 * 3 * PTS * ROWS, 128), F32),
            pltpu.VMEM((SLABS, ROWS, 256), F32),
            pltpu.VMEM((SLABS, ROWS, 256), F32),
            pltpu.VMEM((SLABS, ROWS, 256), F32),
            pltpu.VMEM((2 * C1 * C2, 128), F32),
        ),
    )
    got = lax.all_to_all(sent, "py", split_axis=0, concat_axis=0, tiled=True)
    sent = call(
        second_back_kernel, shape(GX, 48, 128), got, *[jnp.asarray(t) for t in second_back()]
    )
    got = lax.all_to_all(sent, "px", split_axis=0, concat_axis=0, tiled=True)
    tendency = call(
        first_back_kernel, shape(2, 3, Q2, Q3, N1), got, *first,
        scratch=(pltpu.VMEM((N1, 128), F32),),
    )
    return tendency, theta


def solution(mesh):
    in_specs = (P(None, None, "px", "py", None), P("px", "py", None))
    out_specs = (P(None, None, "px", "py", None), P("px", "py", None))
    return jax.shard_map(body, mesh=mesh, in_specs=in_specs, out_specs=out_specs, check_vma=False)
```

```python
import math

import jax
import jax.numpy as jnp
import numpy as np
from jax import lax
from jax.experimental import pallas as pl
from jax.experimental.pallas import tpu as pltpu
from jax.sharding import PartitionSpec as P

NSUB = 3
STEP_RATIO = 0.08
DIFFUSION_RATIO = 1.0
INTERPRET = False

N1, N2, N3 = 512, 128, 128
GX, GY = 32, 8
Q2, Q3 = N2 // GX, N3 // GY
C1, C2 = N1 // GX, N2 // GY
FACTOR = 1.0 / math.sqrt(N1 * N2 * N3)
BF = jnp.bfloat16
F32 = jnp.float32


def halves(table):
    high = table.astype(np.float32).astype(BF)
    low = (table - high.astype(np.float64)).astype(np.float32).astype(BF)
    return np.asarray(high), np.asarray(low)


def waves_np(n):
    index = np.arange(n)
    return 2.0 * math.pi / n * np.where(index < n // 2, index, index - n)


def angles(n):
    index = np.arange(n)
    return 2.0 * math.pi / n * (np.outer(index, index) % n)


def first_table():
    a = angles(N1)
    return halves(np.concatenate([np.cos(a), np.sin(a)], axis=1))


def second_forward():
    a = angles(N2)
    plain = np.zeros((2, N2, N2, 2))
    plain[0, :, :, 0] = np.cos(a)
    plain[0, :, :, 1] = -np.sin(a)
    plain[1, :, :, 0] = np.sin(a)
    plain[1, :, :, 1] = np.cos(a)
    turned = np.zeros_like(plain)
    turned[0] = -plain[1]
    turned[1] = plain[0]
    both = np.stack([plain, turned]).reshape(2, 2 * N2, 2 * N2)
    return halves(both)


def third_forward():
    a = angles(N3)
    return halves(FACTOR * np.concatenate([np.cos(a), -np.sin(a)], axis=0))


def third_back():
    a = angles(N3)
    return halves(FACTOR * np.concatenate([np.cos(a), -np.sin(a)], axis=1))


def second_back():
    a = angles(N2)
    table = np.zeros((N2, 2, 2, N2))
    table[:, 0, 0] = np.cos(a)
    table[:, 0, 1] = np.sin(a)
    table[:, 1, 0] = -np.sin(a)
    table[:, 1, 1] = np.cos(a)
    return halves(table.reshape(2 * N2, 2 * N2))


def split(x):
    high = x.astype(BF)
    return high, (x - high.astype(F32)).astype(BF)


def dots(pairs, dims):
    total = None
    for left, right in pairs:
        part = lax.dot_general(left, right, (dims, ((), ())), preferred_element_type=F32)
        total = part if total is None else total + part
    return total


def dot3(left, right, dims=((1,), (0,))):
    lh, ll = left
    rh, rl = right
    return dots([(lh, rl), (ll, rh), (lh, rh)], dims)


def swap_groups(v):
    lane = lax.broadcasted_iota(jnp.int32, v[0].shape, len(v[0].shape) - 1) // 16
    axis = len(v[0].shape) - 1
    v = list(v)
    for s in (1, 2, 4):
        upper = (lane // s) % 2 == 1
        for i in range(8):
            if i & s:
                continue
            a, b = v[i], v[i + s]
            v[i] = jnp.where(upper, pltpu.roll(b, 16 * s, axis), a)
            v[i + s] = jnp.where(upper, b, pltpu.roll(a, 128 - 16 * s, axis))
    return v


def first_kernel(spec, wave, th, tl, x_low, x_high, out, y):
    rows = []
    for f in (0, 1, 2, 1, 2):
        plain, turned = [], []
        for r in range(Q2):
            re, im = spec[0, f, r], spec[1, f, r]
            plain += [re, im]
            turned += [-im, re]
        piece = jnp.concatenate(
            [jnp.concatenate(plain, axis=0), jnp.concatenate(turned, axis=0)], axis=1
        )
        rows.append(piece if len(rows) < 3 else piece * wave[...])
    table = (th[...], tl[...])
    z = dot3(table, split(jnp.concatenate(rows, axis=0)), ((1,), (1,)))
    for f in range(5):
        y[N1 * f : N1 * f + N1, :] = z[:, 128 * f : 128 * f + 128]
    for f in range(5):
        w = swap_groups([y[pl.ds(N1 * f + i, N1 // 8, stride=8), :] for i in range(8)])
        for g in range(8):
            y[pl.ds(N1 * f + g, N1 // 8, stride=8), :] = w[g]
        out[:, 16 * f : 16 * f + 16, :] = y[N1 * f : N1 * f + N1, :].reshape(GX, 16, 128)


def second_kernel(got, wave2, wave3, th, tl, brick, out):
    c = []
    for f in range(5):
        halves_ = [got[:, 16 * f + 8 * h : 16 * f + 8 * h + 8, :].reshape(256, 128) for h in range(2)]
        c.append(jnp.concatenate(halves_, axis=1))
    k2 = wave2[...]
    k3 = wave3[...]
    curl = [k2 * c[2] - k3 * c[1], k3 * c[0] - c[4], c[3] - k2 * c[0]]
    z = []
    for group, fields in enumerate((c[:3], curl)):
        data = split(jnp.concatenate(fields, axis=1))
        z.append(dot3((th[group], tl[group]), data))
    for f in range(6):
        for ri in range(2):
            for h in range(2):
                at = ((f * 2 + ri) * 2 + h) * 16
                col = (f % 3) * 256 + h * 128
                piece = z[f // 3][ri * 128 : ri * 128 + 128, col : col + 128]
                out[:, at : at + 16, :] = piece.reshape(GY, 16, 128)


def third_kernel(got, th, tl, velocity, vorticity):
    for f in range(6):
        lines = []
        for ri in range(2):
            blocks = []
            for h in range(2):
                at = ((f * 2 + ri) * 2 + h) * 16
                blocks += swap_groups([got[q, at : at + 16, :] for q in range(GY)])
            lines.append(jnp.concatenate(blocks, axis=0))
        u = dot3(split(jnp.concatenate(lines, axis=1)), (th[...], tl[...]))
        out = velocity if f < 3 else vorticity
        out[f % 3] = u.reshape(C1, C2, N3)


def force_lines(velocity, vorticity, b, th, tl, out):
    u = [velocity[i].reshape(C1 * C2, N3) for i in range(3)]
    w = [vorticity[i].reshape(C1 * C2, N3) for i in range(3)]
    force = [u[1] * w[2] - u[2] * w[1], u[2] * w[0] - u[0] * w[2], u[0] * w[1] - u[1] * w[0] + b]
    for f in range(3):
        lines = dot3(split(force[f]), (th[...], tl[...]))
        for ri in range(2):
            for h in range(2):
                at = ((f * 2 + ri) * 2 + h) * 16
                v = [
                    lines[(h * 8 + i) * 16 : (h * 8 + i) * 16 + 16, ri * 128 : ri * 128 + 128]
                    for i in range(8)
                ]
                w8 = swap_groups(v)
                for q in range(GY):
                    out[q, at : at + 16, :] = w8[q]


def parted(table):
    return np.concatenate([table[:, 0::2], table[:, 1::2]], axis=1).astype(np.float32).astype(BF)


def rise_tables():
    plain = np.zeros((N3, 2 * N3))
    for i in range(N3):
        plain[i, 2 * i] += 1.0
        for near in (i, (i + 1) % N3):
            plain[near, 2 * i + 1] += 9.0 / 16.0
        for far in ((i - 1) % N3, (i + 2) % N3):
            plain[far, 2 * i + 1] -= 1.0 / 16.0
    face = 0.5 * (plain + np.roll(plain, -1, axis=1))
    return np.stack([parted(plain), parted(face)])


def parity_tables():
    part = parted(np.eye(2 * N3))
    return part, np.ascontiguousarray(part.T)


def three(x):
    high, rest = x.astype(BF), None
    rest = x - high.astype(F32)
    mid = rest.astype(BF)
    return (rest - mid.astype(F32)).astype(BF), mid, high


def permuted(x, table):
    return dots([(part, table) for part in three(x)], ((1,), (0,)))


def middle(a, b, c, d):
    return (9.0 * (b + c) - (a + d)) * (1.0 / 16.0)


def limited(first, second):
    return jnp.maximum(jnp.minimum(second, 0.0), jnp.minimum(first, jnp.maximum(second, 0.0)))


def upwind(face, left, right, jump):
    return face * jnp.where(face > 0.0, left, right) - DIFFUSION_RATIO * jump


def row_divergence(theta, face):
    count = theta.shape[0]
    jump = pltpu.roll(theta, count - 1, 0) - theta
    half = 0.5 * limited(pltpu.roll(jump, 1, 0), jump)
    flux = upwind(face, theta + half, pltpu.roll(theta - half, count - 1, 0), jump)
    return flux - pltpu.roll(flux, 1, 0)


def lane_divergence(even, odd, face_even, face_odd):
    jump_even = odd - even
    jump_odd = pltpu.roll(even, N3 - 1, 1) - odd
    half_even = 0.5 * limited(even - pltpu.roll(odd, 1, 1), jump_even)
    half_odd = 0.5 * limited(jump_even, jump_odd)
    flux_even = upwind(face_even, even + half_even, odd - half_odd, jump_even)
    flux_odd = upwind(face_odd, odd + half_odd, pltpu.roll(even - half_even, N3 - 1, 1), jump_odd)
    return flux_even - pltpu.roll(flux_odd, 1, 1), flux_odd - flux_even


EDGE = 6
SLABS = 2 * C1 + 2 * EDGE
ROWS = 2 * C2 + 16
PTS = C1 + 8
PROWS = C2 + 16


def brick_kernel(scalar, x_low, x_high, y_low, y_high, table, brick, raw):
    raw[0:EDGE, 8:40, :] = x_low[...]
    raw[EDGE : EDGE + 2 * C1, 8:40, :] = scalar[...]
    raw[EDGE + 2 * C1 :, 8:40, :] = x_high[...]
    at = 0
    for layer in range(3):
        first, count = 2 + 2 * layer, 40 - 4 * layer
        raw[first : first + count, 6 - 2 * layer : 8 - 2 * layer, :] = y_low[at : at + count]
        raw[first : first + count, 40 + 2 * layer : 42 + 2 * layer, :] = y_high[at : at + count]
        at += count

    def part(n, carry):
        z = permuted(raw[pl.ds(4 * n, 4)].reshape(4 * ROWS, 256), table[...])
        for h in range(2):
            brick[pl.ds(4 * n, 4), h] = z[:, h * 128 : h * 128 + 128].reshape(4, ROWS, 128)
        return carry

    lax.fori_loop(0, SLABS // 4, part, 0)


def scalar_kernel(
    brick, velocity, vx_low, vx_high, vy_low, vy_high, vorticity,
    rise, join, th, tl,
    advanced, out,
    ta, tb, last, vw, su, sf, f1, f2, f3, bs,
):
    for c in range(3):
        vw[c * PTS : c * PTS + 4, 8:24, :] = vx_low[c]
        vw[c * PTS + 4 : c * PTS + 20, 8:24, :] = velocity[c]
        vw[c * PTS + 20 : c * PTS + 24, 8:24, :] = vx_high[c]
        vw[c * PTS : c * PTS + 24, 4:8, :] = vy_low[c]
        vw[c * PTS : c * PTS + 24, 24:28, :] = vy_high[c]
    total = 3 * PTS * PROWS
    for c in range(3):
        table = rise[1 if c == 2 else 0]

        def third(n, carry, c=c, table=table):
            lines = vw[pl.ds(c * PTS + 8 * n, 8)].reshape(8 * PROWS, N3)
            high, low = split(lines)
            z = dots([(low, table), (high, table)], ((1,), (0,)))
            at = pl.multiple_of((c * PTS + 8 * n) * PROWS, 8)
            for h in range(2):
                su[pl.ds(h * total + at, 8 * PROWS), :] = z[:, h * 128 : h * 128 + 128]
            return carry

        lax.fori_loop(0, PTS // 8, third, 0)

    def second(n, carry, c):
        for h in range(2):
            at = pl.multiple_of(h * total + (c * PTS + n) * PROWS, 8)
            p = su[pl.ds(at, PROWS), :]
            a, b, cc, d = (p[4 + o : 25 + o] for o in range(4))
            odd, even = middle(a, b, cc, d), cc
            to = (h * 3 * PTS + c * PTS + n) * ROWS
            if c == 1:
                sf[pl.ds(to + 3, 21, stride=2), :] = 0.5 * (odd + even)
                sf[pl.ds(to + 2, 21, stride=2), :] = 0.5 * (b + odd)
            else:
                sf[pl.ds(to + 3, 21, stride=2), :] = odd
                sf[pl.ds(to + 4, 21, stride=2), :] = even
        return carry

    for c in range(3):
        lax.fori_loop(0, PTS, lambda n, k, c=c: second(n, k, c), 0)

    def first(k, carry):
        for c, face in enumerate((f1, f2, f3)):
            for h in range(2):
                a, b, cc, d = (
                    sf[pl.ds(pl.multiple_of((h * 3 * PTS + c * PTS + k + o) * ROWS, 8), ROWS), :]
                    for o in range(4)
                )
                odd = middle(a, b, cc, d)
                if c == 0:
                    face[2 * k + 1, h] = 0.5 * (odd + cc)
                    face[2 * k, h] = 0.5 * (b + odd)
                else:
                    face[2 * k + 1, h] = odd
                    face[2 * k + 2, h] = cc
        return carry

    lax.fori_loop(0, 21, first, 0)

    for turn, (source, target) in enumerate(((brick, ta), (ta, tb), (tb, last))):
        low = 2 + 2 * turn
        begin = []
        for h in range(2):
            t0, t1, t2, t3 = (source[low - 2 + o, h] for o in range(4))
            j0, j1, j2 = t1 - t0, t2 - t1, t3 - t2
            h1, h2 = 0.5 * limited(j0, j1), 0.5 * limited(j1, j2)
            begin.append((t2 + h2, j2, upwind(f1[low - 1, h], t1 + h1, t2 - h2, j1)))

        def step(i, carry, source=source, target=target, turn=turn):
            here = [source[i, h] for h in range(2)]
            change = list(lane_divergence(*here, f3[i, 0], f3[i, 1]))
            done = []
            for h in range(2):
                left, jump, before = carry[h]
                ahead = source[i + 1, h]
                next_jump = source[i + 2, h] - ahead
                half = 0.5 * limited(jump, next_jump)
                flux = upwind(f1[i, h], left, ahead - half, jump)
                total = change[h] + (flux - before) + row_divergence(here[h], f2[i, h])
                fresh = here[h] - STEP_RATIO * total
                if turn < NSUB - 1:
                    target[i, h] = fresh
                else:
                    target[i - EDGE, :, h * 128 : h * 128 + 128] = fresh[8:40]
                done.append((ahead + half, next_jump, flux))
            return tuple(done)

        lax.fori_loop(low, SLABS - low, step, tuple(begin))

    def finish(n, carry):
        lines = last[pl.ds(4 * n, 4)]
        advanced[pl.ds(4 * n, 4)] = permuted(lines.reshape(128, 256), join[...]).reshape(4, 32, 256)
        both = lines[:, :, :128] + lines[:, :, 128:]
        bs[pl.ds(pl.multiple_of(64 * n, 8), 32), :] = 0.125 * (both[0] + both[1])
        bs[pl.ds(pl.multiple_of(64 * n + 32, 8), 32), :] = 0.125 * (both[2] + both[3])
        return carry

    lax.fori_loop(0, C1 // 2, finish, 0)
    buoyancy = bs[pl.ds(0, C1 * C2, stride=2), :] + bs[pl.ds(1, C1 * C2, stride=2), :]
    force_lines(velocity, vorticity, buoyancy, th, tl, out)


def second_back_kernel(got, th, tl, out):
    columns = []
    for f in range(3):
        for h in range(2):
            parts = []
            for ri in range(2):
                at = ((f * 2 + ri) * 2 + h) * 16
                parts.append(got[:, at : at + 16, :].reshape(128, 128))
            columns.append(jnp.concatenate(parts, axis=0))
    z = dot3((th[...], tl[...]), split(jnp.concatenate(columns, axis=1)))
    for f in range(3):
        for h in range(2):
            at = f * 16 + h * 8
            col = (f * 2 + h) * 128
            out[:, at : at + 8, :] = z[:, col : col + 128].reshape(GX, 8, 128)


def first_back_kernel(got, th, tl, out, y):
    rows = []
    for f in range(3):
        y[...] = got[:, 16 * f : 16 * f + 16, :].reshape(N1, 128)
        w = swap_groups([y[pl.ds(g, N1 // 8, stride=8), :] for g in range(8)])
        for i in range(8):
            y[pl.ds(i, N1 // 8, stride=8), :] = w[i]
        rows.append(y[...].T)
    z = dot3(split(jnp.concatenate(rows, axis=0)), (th[...], tl[...]))
    for f in range(3):
        for r in range(Q2):
            at = f * 128 + r * 32
            cr, ci = z[at : at + 16, :N1], z[at + 16 : at + 32, :N1]
            sr, si = z[at : at + 16, N1:], z[at + 16 : at + 32, N1:]
            out[0, f, r] = cr + si
            out[1, f, r] = ci - sr


def call(kernel, out_shape, *args, scratch=(), late=0):
    specs = [pl.BlockSpec(memory_space=pltpu.VMEM)] * (len(args) - late)
    specs += [pl.BlockSpec(memory_space=pl.ANY)] * late
    return pl.pallas_call(
        kernel,
        in_specs=specs,
        out_shape=out_shape,
        scratch_shapes=list(scratch),
        interpret=INTERPRET,
        name=kernel.__name__,
        compiler_params=pltpu.CompilerParams(vmem_limit_bytes=48 * 1024 * 1024),
    )(*args)


def shape(*dims):
    return jax.ShapeDtypeStruct(dims, F32)


def ring(axis):
    count = lax.axis_size(axis)
    up = [(i, (i + 1) % count) for i in range(count)]
    return up, [(b, a) for a, b in up]


def edges(axis, first, last):
    up, down = ring(axis)
    return lax.ppermute(last, axis, up), lax.ppermute(first, axis, down)


def body(spectrum, scalar):
    wave_first = np.tile(waves_np(N1).astype(np.float32), 2)[None]
    wave_second = np.repeat(waves_np(N2).astype(np.float32), 2)[:, None]
    blocks = np.tile(waves_np(N3).astype(np.float32).reshape(GY, 1, Q3), (1, 16, 1)).reshape(GY, 1, 256)
    wave_third = lax.dynamic_index_in_dim(jnp.asarray(blocks), lax.axis_index("py"), 0, keepdims=False)
    first = [jnp.asarray(t) for t in first_table()]
    second = [jnp.asarray(t) for t in second_forward()]
    third = [jnp.asarray(t) for t in third_forward()]
    x_low, x_high = edges("px", scalar[:EDGE], scalar[-EDGE:])
    around = jnp.concatenate([x_low[2:], scalar, x_high[:4]], axis=0)
    strips = [
        jnp.concatenate([around[2 * n : 40 - 2 * n, at : at + 2] for n, at in enumerate(starts)], axis=0)
        for starts in ((0, 2, 4), (2 * C2 - 2, 2 * C2 - 4, 2 * C2 - 6))
    ]
    y_low, y_high = edges("py", *strips)
    part, join = (jnp.asarray(t) for t in parity_tables())
    brick = call(
        brick_kernel, shape(SLABS, 2, ROWS, 128), scalar, x_low, x_high, y_low, y_high, part,
        scratch=(pltpu.VMEM((SLABS, ROWS, 256), F32),),
    )
    sent = call(
        first_kernel, shape(GX, 80, 128), spectrum, jnp.asarray(wave_first), *first, x_low, x_high,
        scratch=(pltpu.VMEM((5 * N1, 128), F32),), late=2,
    )
    got = lax.all_to_all(sent, "px", split_axis=0, concat_axis=0, tiled=True)
    sent = call(second_kernel, shape(GY, 384, 128), got, jnp.asarray(wave_second), wave_third, *second, brick, late=1)
    got = lax.all_to_all(sent, "py", split_axis=0, concat_axis=0, tiled=True)
    velocity, vorticity = call(
        third_kernel, (shape(3, C1, C2, N3), shape(3, C1, C2, N3)), got, *third
    )
    vx_low, vx_high = edges("px", velocity[:, :4], velocity[:, -4:])
    strips = [
        jnp.concatenate([part[:, :, cut] for part in (vx_low, velocity, vx_high)], axis=1)
        for cut in (slice(0, 4), slice(C2 - 4, C2))
    ]
    vy_low, vy_high = edges("py", *strips)
    theta, sent = call(
        scalar_kernel, (shape(2 * C1, 2 * C2, 2 * N3), shape(GY, 192, 128)),
        brick, velocity, vx_low, vx_high, vy_low, vy_high, vorticity,
        jnp.asarray(rise_tables()), join, *[jnp.asarray(t) for t in third_back()],
        scratch=(
            pltpu.VMEM((SLABS, 2, ROWS, 128), F32),
            pltpu.VMEM((SLABS, 2, ROWS, 128), F32),
            pltpu.VMEM((2 * C1, 2 * C2, 256), F32),
            pltpu.VMEM((3 * PTS, PROWS, N3), F32),
            pltpu.VMEM((2 * 3 * PTS * PROWS, 128), F32),
            pltpu.VMEM((2 * 3 * PTS * ROWS, 128), F32),
            pltpu.VMEM((SLABS, 2, ROWS, 128), F32),
            pltpu.VMEM((SLABS, 2, ROWS, 128), F32),
            pltpu.VMEM((SLABS, 2, ROWS, 128), F32),
            pltpu.VMEM((2 * C1 * C2, 128), F32),
        ),
    )
    got = lax.all_to_all(sent, "py", split_axis=0, concat_axis=0, tiled=True)
    sent = call(
        second_back_kernel, shape(GX, 48, 128), got, *[jnp.asarray(t) for t in second_back()]
    )
    got = lax.all_to_all(sent, "px", split_axis=0, concat_axis=0, tiled=True)
    tendency = call(
        first_back_kernel, shape(2, 3, Q2, Q3, N1), got, *first,
        scratch=(pltpu.VMEM((N1, 128), F32),),
    )
    return tendency, theta


def solution(mesh):
    in_specs = (P(None, None, "px", "py", None), P("px", "py", None))
    out_specs = (P(None, None, "px", "py", None), P("px", "py", None))
    return jax.shard_map(body, mesh=mesh, in_specs=in_specs, out_specs=out_specs, check_vma=False)
```

```python
import math

import jax
import jax.numpy as jnp
import numpy as np
from jax import lax
from jax.experimental import pallas as pl
from jax.experimental.pallas import tpu as pltpu
from jax.sharding import PartitionSpec as P

NSUB = 3
STEP_RATIO = 0.08
DIFFUSION_RATIO = 1.0
INTERPRET = False

N1, N2, N3 = 512, 128, 128
GX, GY = 32, 8
Q2, Q3 = N2 // GX, N3 // GY
C1, C2 = N1 // GX, N2 // GY
FACTOR = 1.0 / math.sqrt(N1 * N2 * N3)
BF = jnp.bfloat16
F32 = jnp.float32


def halves(table):
    high = table.astype(np.float32).astype(BF)
    low = (table - high.astype(np.float64)).astype(np.float32).astype(BF)
    return np.asarray(high), np.asarray(low)


def waves_np(n):
    index = np.arange(n)
    return 2.0 * math.pi / n * np.where(index < n // 2, index, index - n)


def angles(n):
    index = np.arange(n)
    return 2.0 * math.pi / n * (np.outer(index, index) % n)


def first_table():
    a = angles(N1)
    return halves(np.concatenate([np.cos(a), np.sin(a)], axis=1))


def second_forward():
    a = angles(N2)
    plain = np.zeros((2, N2, N2, 2))
    plain[0, :, :, 0] = np.cos(a)
    plain[0, :, :, 1] = -np.sin(a)
    plain[1, :, :, 0] = np.sin(a)
    plain[1, :, :, 1] = np.cos(a)
    turned = np.zeros_like(plain)
    turned[0] = -plain[1]
    turned[1] = plain[0]
    both = np.stack([plain, turned]).reshape(2, 2 * N2, 2 * N2)
    return halves(both)


def third_forward():
    a = angles(N3)
    return halves(FACTOR * np.concatenate([np.cos(a), -np.sin(a)], axis=0))


def third_back():
    a = angles(N3)
    return halves(FACTOR * np.concatenate([np.cos(a), -np.sin(a)], axis=1))


def second_back():
    a = angles(N2)
    table = np.zeros((N2, 2, 2, N2))
    table[:, 0, 0] = np.cos(a)
    table[:, 0, 1] = np.sin(a)
    table[:, 1, 0] = -np.sin(a)
    table[:, 1, 1] = np.cos(a)
    return halves(table.reshape(2 * N2, 2 * N2))


def split(x):
    high = x.astype(BF)
    return high, (x - high.astype(F32)).astype(BF)


def dots(pairs, dims):
    total = None
    for left, right in pairs:
        part = lax.dot_general(left, right, (dims, ((), ())), preferred_element_type=F32)
        total = part if total is None else total + part
    return total


def dot3(left, right, dims=((1,), (0,))):
    lh, ll = left
    rh, rl = right
    return dots([(lh, rl), (ll, rh), (lh, rh)], dims)


def swap_groups(v):
    lane = lax.broadcasted_iota(jnp.int32, v[0].shape, len(v[0].shape) - 1) // 16
    axis = len(v[0].shape) - 1
    v = list(v)
    for s in (1, 2, 4):
        upper = (lane // s) % 2 == 1
        for i in range(8):
            if i & s:
                continue
            a, b = v[i], v[i + s]
            v[i] = jnp.where(upper, pltpu.roll(b, 16 * s, axis), a)
            v[i + s] = jnp.where(upper, b, pltpu.roll(a, 128 - 16 * s, axis))
    return v


def first_kernel(spec, wave, th, tl, out, y):
    rows = []
    for f in (0, 1, 2, 1, 2):
        plain, turned = [], []
        for r in range(Q2):
            re, im = spec[0, f, r], spec[1, f, r]
            plain += [re, im]
            turned += [-im, re]
        piece = jnp.concatenate(
            [jnp.concatenate(plain, axis=0), jnp.concatenate(turned, axis=0)], axis=1
        )
        rows.append(piece if len(rows) < 3 else piece * wave[...])
    table = (th[...], tl[...])
    z = dot3(table, split(jnp.concatenate(rows, axis=0)), ((1,), (1,)))
    for f in range(5):
        y[N1 * f : N1 * f + N1, :] = z[:, 128 * f : 128 * f + 128]
    for f in range(5):
        w = swap_groups([y[pl.ds(N1 * f + i, N1 // 8, stride=8), :] for i in range(8)])
        for g in range(8):
            y[pl.ds(N1 * f + g, N1 // 8, stride=8), :] = w[g]
        out[:, 16 * f : 16 * f + 16, :] = y[N1 * f : N1 * f + N1, :].reshape(GX, 16, 128)


def second_kernel(got, wave2, wave3, th, tl, x_low, x_high, out):
    c = []
    for f in range(5):
        halves_ = [got[:, 16 * f + 8 * h : 16 * f + 8 * h + 8, :].reshape(256, 128) for h in range(2)]
        c.append(jnp.concatenate(halves_, axis=1))
    k2 = wave2[...]
    k3 = wave3[...]
    curl = [k2 * c[2] - k3 * c[1], k3 * c[0] - c[4], c[3] - k2 * c[0]]
    z = []
    for group, fields in enumerate((c[:3], curl)):
        data = split(jnp.concatenate(fields, axis=1))
        z.append(dot3((th[group], tl[group]), data))
    for f in range(6):
        for ri in range(2):
            for h in range(2):
                at = ((f * 2 + ri) * 2 + h) * 16
                col = (f % 3) * 256 + h * 128
                piece = z[f // 3][ri * 128 : ri * 128 + 128, col : col + 128]
                out[:, at : at + 16, :] = piece.reshape(GY, 16, 128)


def third_kernel(got, th, tl, velocity, vorticity):
    for f in range(6):
        lines = []
        for ri in range(2):
            blocks = []
            for h in range(2):
                at = ((f * 2 + ri) * 2 + h) * 16
                blocks += swap_groups([got[q, at : at + 16, :] for q in range(GY)])
            lines.append(jnp.concatenate(blocks, axis=0))
        u = dot3(split(jnp.concatenate(lines, axis=1)), (th[...], tl[...]))
        out = velocity if f < 3 else vorticity
        out[f % 3] = u.reshape(C1, C2, N3)


def force_lines(velocity, vorticity, b, th, tl, out):
    u = [velocity[i].reshape(C1 * C2, N3) for i in range(3)]
    w = [vorticity[i].reshape(C1 * C2, N3) for i in range(3)]
    force = [u[1] * w[2] - u[2] * w[1], u[2] * w[0] - u[0] * w[2], u[0] * w[1] - u[1] * w[0] + b]
    for f in range(3):
        lines = dot3(split(force[f]), (th[...], tl[...]))
        for ri in range(2):
            for h in range(2):
                at = ((f * 2 + ri) * 2 + h) * 16
                v = [
                    lines[(h * 8 + i) * 16 : (h * 8 + i) * 16 + 16, ri * 128 : ri * 128 + 128]
                    for i in range(8)
                ]
                w8 = swap_groups(v)
                for q in range(GY):
                    out[q, at : at + 16, :] = w8[q]


def parted(table):
    return np.concatenate([table[:, 0::2], table[:, 1::2]], axis=1).astype(np.float32).astype(BF)


def rise_tables():
    plain = np.zeros((N3, 2 * N3))
    for i in range(N3):
        plain[i, 2 * i] += 1.0
        for near in (i, (i + 1) % N3):
            plain[near, 2 * i + 1] += 9.0 / 16.0
        for far in ((i - 1) % N3, (i + 2) % N3):
            plain[far, 2 * i + 1] -= 1.0 / 16.0
    face = 0.5 * (plain + np.roll(plain, -1, axis=1))
    return np.stack([parted(plain), parted(face)])


def parity_tables():
    part = parted(np.eye(2 * N3))
    return part, np.ascontiguousarray(part.T)


def three(x):
    high, rest = x.astype(BF), None
    rest = x - high.astype(F32)
    mid = rest.astype(BF)
    return (rest - mid.astype(F32)).astype(BF), mid, high


def permuted(x, table):
    return dots([(part, table) for part in three(x)], ((1,), (0,)))


def middle(a, b, c, d):
    return (9.0 * (b + c) - (a + d)) * (1.0 / 16.0)


def limited(first, second):
    return jnp.maximum(jnp.minimum(second, 0.0), jnp.minimum(first, jnp.maximum(second, 0.0)))


def upwind(face, left, right, jump):
    return face * jnp.where(face > 0.0, left, right) - DIFFUSION_RATIO * jump


def row_divergence(theta, face):
    count = theta.shape[0]
    jump = pltpu.roll(theta, count - 1, 0) - theta
    half = 0.5 * limited(pltpu.roll(jump, 1, 0), jump)
    flux = upwind(face, theta + half, pltpu.roll(theta - half, count - 1, 0), jump)
    return flux - pltpu.roll(flux, 1, 0)


def lane_divergence(even, odd, face_even, face_odd):
    jump_even = odd - even
    jump_odd = pltpu.roll(even, N3 - 1, 1) - odd
    half_even = 0.5 * limited(even - pltpu.roll(odd, 1, 1), jump_even)
    half_odd = 0.5 * limited(jump_even, jump_odd)
    flux_even = upwind(face_even, even + half_even, odd - half_odd, jump_even)
    flux_odd = upwind(face_odd, odd + half_odd, pltpu.roll(even - half_even, N3 - 1, 1), jump_odd)
    return flux_even - pltpu.roll(flux_odd, 1, 1), flux_odd - flux_even


EDGE = 6
SLABS = 2 * C1 + 2 * EDGE
ROWS = 2 * C2 + 16
PTS = C1 + 8
PROWS = C2 + 16


def brick_kernel(scalar, x_low, x_high, y_low, y_high, table, brick, raw):
    raw[0:EDGE, 8:40, :] = x_low[...]
    raw[EDGE : EDGE + 2 * C1, 8:40, :] = scalar[...]
    raw[EDGE + 2 * C1 :, 8:40, :] = x_high[...]
    at = 0
    for layer in range(3):
        first, count = 2 + 2 * layer, 40 - 4 * layer
        raw[first : first + count, 6 - 2 * layer : 8 - 2 * layer, :] = y_low[at : at + count]
        raw[first : first + count, 40 + 2 * layer : 42 + 2 * layer, :] = y_high[at : at + count]
        at += count

    def part(n, carry):
        z = permuted(raw[pl.ds(4 * n, 4)].reshape(4 * ROWS, 256), table[...])
        for h in range(2):
            brick[pl.ds(4 * n, 4), h] = z[:, h * 128 : h * 128 + 128].reshape(4, ROWS, 128)
        return carry

    lax.fori_loop(0, SLABS // 4, part, 0)


def scalar_kernel(
    brick, velocity, vx_low, vx_high, vy_low, vy_high, vorticity,
    rise, join, th, tl,
    advanced, out,
    ta, tb, last, vw, su, sf, f1, f2, f3, bs,
):
    for c in range(3):
        vw[c * PTS : c * PTS + 4, 8:24, :] = vx_low[c]
        vw[c * PTS + 4 : c * PTS + 20, 8:24, :] = velocity[c]
        vw[c * PTS + 20 : c * PTS + 24, 8:24, :] = vx_high[c]
        vw[c * PTS : c * PTS + 24, 4:8, :] = vy_low[c]
        vw[c * PTS : c * PTS + 24, 24:28, :] = vy_high[c]
    total = 3 * PTS * PROWS
    for c in range(3):
        table = rise[1 if c == 2 else 0]

        def third(n, carry, c=c, table=table):
            lines = vw[pl.ds(c * PTS + 8 * n, 8)].reshape(8 * PROWS, N3)
            high, low = split(lines)
            z = dots([(low, table), (high, table)], ((1,), (0,)))
            at = pl.multiple_of((c * PTS + 8 * n) * PROWS, 8)
            for h in range(2):
                su[pl.ds(h * total + at, 8 * PROWS), :] = z[:, h * 128 : h * 128 + 128]
            return carry

        lax.fori_loop(0, PTS // 8, third, 0)

    def second(n, carry, c):
        for h in range(2):
            at = pl.multiple_of(h * total + (c * PTS + n) * PROWS, 8)
            p = su[pl.ds(at, PROWS), :]
            a, b, cc, d = (p[4 + o : 25 + o] for o in range(4))
            odd, even = middle(a, b, cc, d), cc
            to = (h * 3 * PTS + c * PTS + n) * ROWS
            if c == 1:
                sf[pl.ds(to + 3, 21, stride=2), :] = 0.5 * (odd + even)
                sf[pl.ds(to + 2, 21, stride=2), :] = 0.5 * (b + odd)
            else:
                sf[pl.ds(to + 3, 21, stride=2), :] = odd
                sf[pl.ds(to + 4, 21, stride=2), :] = even
        return carry

    for c in range(3):
        lax.fori_loop(0, PTS, lambda n, k, c=c: second(n, k, c), 0)

    def first(k, carry):
        for c, face in enumerate((f1, f2, f3)):
            for h in range(2):
                a, b, cc, d = (
                    sf[pl.ds(pl.multiple_of((h * 3 * PTS + c * PTS + k + o) * ROWS, 8), ROWS), :]
                    for o in range(4)
                )
                odd = middle(a, b, cc, d)
                if c == 0:
                    face[2 * k + 1, h] = 0.5 * (odd + cc)
                    face[2 * k, h] = 0.5 * (b + odd)
                else:
                    face[2 * k + 1, h] = odd
                    face[2 * k + 2, h] = cc
        return carry

    lax.fori_loop(0, 21, first, 0)

    for turn, (source, target) in enumerate(((brick, ta), (ta, tb), (tb, last))):
        low = 2 + 2 * turn
        begin = []
        for h in range(2):
            t0, t1, t2, t3 = (source[low - 2 + o, h] for o in range(4))
            j0, j1, j2 = t1 - t0, t2 - t1, t3 - t2
            h1, h2 = 0.5 * limited(j0, j1), 0.5 * limited(j1, j2)
            begin.append((t2 + h2, j2, upwind(f1[low - 1, h], t1 + h1, t2 - h2, j1)))

        def step(i, carry, source=source, target=target, turn=turn):
            here = [source[i, h] for h in range(2)]
            change = list(lane_divergence(*here, f3[i, 0], f3[i, 1]))
            done = []
            for h in range(2):
                left, jump, before = carry[h]
                ahead = source[i + 1, h]
                next_jump = source[i + 2, h] - ahead
                half = 0.5 * limited(jump, next_jump)
                flux = upwind(f1[i, h], left, ahead - half, jump)
                total = change[h] + (flux - before) + row_divergence(here[h], f2[i, h])
                fresh = here[h] - STEP_RATIO * total
                if turn < NSUB - 1:
                    target[i, h] = fresh
                else:
                    target[i - EDGE, :, h * 128 : h * 128 + 128] = fresh[8:40]
                done.append((ahead + half, next_jump, flux))
            return tuple(done)

        lax.fori_loop(low, SLABS - low, step, tuple(begin))

    def finish(n, carry):
        lines = last[pl.ds(4 * n, 4)]
        advanced[pl.ds(4 * n, 4)] = permuted(lines.reshape(128, 256), join[...]).reshape(4, 32, 256)
        both = lines[:, :, :128] + lines[:, :, 128:]
        bs[pl.ds(pl.multiple_of(64 * n, 8), 32), :] = 0.125 * (both[0] + both[1])
        bs[pl.ds(pl.multiple_of(64 * n + 32, 8), 32), :] = 0.125 * (both[2] + both[3])
        return carry

    lax.fori_loop(0, C1 // 2, finish, 0)
    buoyancy = bs[pl.ds(0, C1 * C2, stride=2), :] + bs[pl.ds(1, C1 * C2, stride=2), :]
    force_lines(velocity, vorticity, buoyancy, th, tl, out)


def second_back_kernel(got, th, tl, out):
    columns = []
    for f in range(3):
        for h in range(2):
            parts = []
            for ri in range(2):
                at = ((f * 2 + ri) * 2 + h) * 16
                parts.append(got[:, at : at + 16, :].reshape(128, 128))
            columns.append(jnp.concatenate(parts, axis=0))
    z = dot3((th[...], tl[...]), split(jnp.concatenate(columns, axis=1)))
    for f in range(3):
        for h in range(2):
            at = f * 16 + h * 8
            col = (f * 2 + h) * 128
            out[:, at : at + 8, :] = z[:, col : col + 128].reshape(GX, 8, 128)


def first_back_kernel(got, th, tl, out, y):
    rows = []
    for f in range(3):
        y[...] = got[:, 16 * f : 16 * f + 16, :].reshape(N1, 128)
        w = swap_groups([y[pl.ds(g, N1 // 8, stride=8), :] for g in range(8)])
        for i in range(8):
            y[pl.ds(i, N1 // 8, stride=8), :] = w[i]
        rows.append(y[...].T)
    z = dot3(split(jnp.concatenate(rows, axis=0)), (th[...], tl[...]))
    for f in range(3):
        for r in range(Q2):
            at = f * 128 + r * 32
            cr, ci = z[at : at + 16, :N1], z[at + 16 : at + 32, :N1]
            sr, si = z[at : at + 16, N1:], z[at + 16 : at + 32, N1:]
            out[0, f, r] = cr + si
            out[1, f, r] = ci - sr


def call(kernel, out_shape, *args, scratch=(), late=0, hbm=False):
    specs = [pl.BlockSpec(memory_space=pltpu.VMEM)] * (len(args) - late)
    specs += [pl.BlockSpec(memory_space=pl.ANY)] * late
    return pl.pallas_call(
        kernel,
        in_specs=specs,
        out_shape=out_shape if not hbm else pltpu.HBM(out_shape.shape, out_shape.dtype),
        out_specs=jax.tree.map(lambda _: pl.BlockSpec(memory_space=pltpu.VMEM), out_shape),
        scratch_shapes=list(scratch),
        interpret=INTERPRET,
        name=kernel.__name__,
        compiler_params=pltpu.CompilerParams(vmem_limit_bytes=48 * 1024 * 1024),
    )(*args)


def shape(*dims):
    return jax.ShapeDtypeStruct(dims, F32)


def ring(axis):
    count = lax.axis_size(axis)
    up = [(i, (i + 1) % count) for i in range(count)]
    return up, [(b, a) for a, b in up]


def edges(axis, first, last):
    up, down = ring(axis)
    return lax.ppermute(last, axis, up), lax.ppermute(first, axis, down)


def body(spectrum, scalar):
    wave_first = np.tile(waves_np(N1).astype(np.float32), 2)[None]
    wave_second = np.repeat(waves_np(N2).astype(np.float32), 2)[:, None]
    blocks = np.tile(waves_np(N3).astype(np.float32).reshape(GY, 1, Q3), (1, 16, 1)).reshape(GY, 1, 256)
    wave_third = lax.dynamic_index_in_dim(jnp.asarray(blocks), lax.axis_index("py"), 0, keepdims=False)
    first = [jnp.asarray(t) for t in first_table()]
    second = [jnp.asarray(t) for t in second_forward()]
    third = [jnp.asarray(t) for t in third_forward()]
    x_low, x_high = edges("px", scalar[:EDGE], scalar[-EDGE:])
    around = jnp.concatenate([x_low[2:], scalar, x_high[:4]], axis=0)
    strips = [
        jnp.concatenate([around[2 * n : 40 - 2 * n, at : at + 2] for n, at in enumerate(starts)], axis=0)
        for starts in ((0, 2, 4), (2 * C2 - 2, 2 * C2 - 4, 2 * C2 - 6))
    ]
    y_low, y_high = edges("py", *strips)
    part, join = (jnp.asarray(t) for t in parity_tables())
    brick = call(
        brick_kernel, shape(SLABS, 2, ROWS, 128), scalar, x_low, x_high, y_low, y_high, part,
        scratch=(pltpu.VMEM((SLABS, ROWS, 256), F32),),
    )
    sent = call(
        first_kernel, shape(GX, 80, 128), spectrum, jnp.asarray(wave_first), *first,
        scratch=(pltpu.VMEM((5 * N1, 128), F32),),
    )
    got = lax.all_to_all(sent, "px", split_axis=0, concat_axis=0, tiled=True)
    sent = call(second_kernel, shape(GY, 384, 128), got, jnp.asarray(wave_second), wave_third, *second, x_low, x_high, late=2, hbm=True)
    got = lax.all_to_all(sent, "py", split_axis=0, concat_axis=0, tiled=True)
    velocity, vorticity = call(
        third_kernel, (shape(3, C1, C2, N3), shape(3, C1, C2, N3)), got, *third
    )
    vx_low, vx_high = edges("px", velocity[:, :4], velocity[:, -4:])
    strips = [
        jnp.concatenate([part[:, :, cut] for part in (vx_low, velocity, vx_high)], axis=1)
        for cut in (slice(0, 4), slice(C2 - 4, C2))
    ]
    vy_low, vy_high = edges("py", *strips)
    theta, sent = call(
        scalar_kernel, (shape(2 * C1, 2 * C2, 2 * N3), shape(GY, 192, 128)),
        brick, velocity, vx_low, vx_high, vy_low, vy_high, vorticity,
        jnp.asarray(rise_tables()), join, *[jnp.asarray(t) for t in third_back()],
        scratch=(
            pltpu.VMEM((SLABS, 2, ROWS, 128), F32),
            pltpu.VMEM((SLABS, 2, ROWS, 128), F32),
            pltpu.VMEM((2 * C1, 2 * C2, 256), F32),
            pltpu.VMEM((3 * PTS, PROWS, N3), F32),
            pltpu.VMEM((2 * 3 * PTS * PROWS, 128), F32),
            pltpu.VMEM((2 * 3 * PTS * ROWS, 128), F32),
            pltpu.VMEM((SLABS, 2, ROWS, 128), F32),
            pltpu.VMEM((SLABS, 2, ROWS, 128), F32),
            pltpu.VMEM((SLABS, 2, ROWS, 128), F32),
            pltpu.VMEM((2 * C1 * C2, 128), F32),
        ),
    )
    got = lax.all_to_all(sent, "py", split_axis=0, concat_axis=0, tiled=True)
    sent = call(
        second_back_kernel, shape(GX, 48, 128), got, *[jnp.asarray(t) for t in second_back()]
    )
    got = lax.all_to_all(sent, "px", split_axis=0, concat_axis=0, tiled=True)
    tendency = call(
        first_back_kernel, shape(2, 3, Q2, Q3, N1), got, *first,
        scratch=(pltpu.VMEM((N1, 128), F32),),
    )
    return tendency, theta


def solution(mesh):
    in_specs = (P(None, None, "px", "py", None), P("px", "py", None))
    out_specs = (P(None, None, "px", "py", None), P("px", "py", None))
    return jax.shard_map(body, mesh=mesh, in_specs=in_specs, out_specs=out_specs, check_vma=False)
```

```python
import math

import jax
import jax.numpy as jnp
import numpy as np
from jax import lax
from jax.experimental import pallas as pl
from jax.experimental.pallas import tpu as pltpu
from jax.sharding import PartitionSpec as P


NSUB = 3
STEP_RATIO = 0.08
DIFFUSION_RATIO = 1.0
INTERPRET = False

N1, N2, N3 = 512, 128, 128
GX, GY = 32, 8
Q2, Q3 = N2 // GX, N3 // GY
C1, C2 = N1 // GX, N2 // GY
FACTOR = 1.0 / math.sqrt(N1 * N2 * N3)
BF = jnp.bfloat16
F32 = jnp.float32


def halves(table):
    high = table.astype(np.float32).astype(BF)
    low = (table - high.astype(np.float64)).astype(np.float32).astype(BF)
    return np.asarray(high), np.asarray(low)


def waves_np(n):
    index = np.arange(n)
    return 2.0 * math.pi / n * np.where(index < n // 2, index, index - n)


def angles(n):
    index = np.arange(n)
    return 2.0 * math.pi / n * (np.outer(index, index) % n)


def first_table():
    a = angles(N1)
    return halves(np.concatenate([np.cos(a), np.sin(a)], axis=1))


def second_forward():
    a = angles(N2)
    plain = np.zeros((2, N2, N2, 2))
    plain[0, :, :, 0] = np.cos(a)
    plain[0, :, :, 1] = -np.sin(a)
    plain[1, :, :, 0] = np.sin(a)
    plain[1, :, :, 1] = np.cos(a)
    turned = np.zeros_like(plain)
    turned[0] = -plain[1]
    turned[1] = plain[0]
    both = np.stack([plain, turned]).reshape(2, 2 * N2, 2 * N2)
    return halves(both)


def third_forward():
    a = angles(N3)
    return halves(FACTOR * np.concatenate([np.cos(a), -np.sin(a)], axis=0))


def third_back():
    a = angles(N3)
    return halves(FACTOR * np.concatenate([np.cos(a), -np.sin(a)], axis=1))


def second_back():
    a = angles(N2)
    table = np.zeros((N2, 2, 2, N2))
    table[:, 0, 0] = np.cos(a)
    table[:, 0, 1] = np.sin(a)
    table[:, 1, 0] = -np.sin(a)
    table[:, 1, 1] = np.cos(a)
    return halves(table.reshape(2 * N2, 2 * N2))


def split(x):
    high = x.astype(BF)
    return high, (x - high.astype(F32)).astype(BF)


def dots(pairs, dims):
    total = None
    for left, right in pairs:
        part = lax.dot_general(left, right, (dims, ((), ())), preferred_element_type=F32)
        total = part if total is None else total + part
    return total


def dot3(left, right, dims=((1,), (0,))):
    lh, ll = left
    rh, rl = right
    return dots([(lh, rl), (ll, rh), (lh, rh)], dims)


def swap_groups(v):
    lane = lax.broadcasted_iota(jnp.int32, v[0].shape, len(v[0].shape) - 1) // 16
    axis = len(v[0].shape) - 1
    v = list(v)
    for s in (1, 2, 4):
        upper = (lane // s) % 2 == 1
        for i in range(8):
            if i & s:
                continue
            a, b = v[i], v[i + s]
            v[i] = jnp.where(upper, pltpu.roll(b, 16 * s, axis), a)
            v[i + s] = jnp.where(upper, b, pltpu.roll(a, 128 - 16 * s, axis))
    return v


def first_kernel(spec, wave, th, tl, out, y):
    rows = []
    for f in (0, 1, 2, 1, 2):
        plain, turned = [], []
        for r in range(Q2):
            re, im = spec[0, f, r], spec[1, f, r]
            plain += [re, im]
            turned += [-im, re]
        piece = jnp.concatenate(
            [jnp.concatenate(plain, axis=0), jnp.concatenate(turned, axis=0)], axis=1
        )
        rows.append(piece if len(rows) < 3 else piece * wave[...])
    table = (th[...], tl[...])
    z = dot3(table, split(jnp.concatenate(rows, axis=0)), ((1,), (1,)))
    for f in range(5):
        y[N1 * f : N1 * f + N1, :] = z[:, 128 * f : 128 * f + 128]
    for f in range(5):
        w = swap_groups([y[pl.ds(N1 * f + i, N1 // 8, stride=8), :] for i in range(8)])
        for g in range(8):
            y[pl.ds(N1 * f + g, N1 // 8, stride=8), :] = w[g]
        out[:, 16 * f : 16 * f + 16, :] = y[N1 * f : N1 * f + N1, :].reshape(GX, 16, 128)


def second_kernel(got, wave2, wave3, th, tl, x_low, x_high, out):
    c = []
    for f in range(5):
        halves_ = [got[:, 16 * f + 8 * h : 16 * f + 8 * h + 8, :].reshape(256, 128) for h in range(2)]
        c.append(jnp.concatenate(halves_, axis=1))
    k2 = wave2[...]
    k3 = wave3[...]
    curl = [k2 * c[2] - k3 * c[1], k3 * c[0] - c[4], c[3] - k2 * c[0]]
    z = []
    for group, fields in enumerate((c[:3], curl)):
        data = split(jnp.concatenate(fields, axis=1))
        z.append(dot3((th[group], tl[group]), data))
    for f in range(6):
        for ri in range(2):
            for h in range(2):
                at = ((f * 2 + ri) * 2 + h) * 16
                col = (f % 3) * 256 + h * 128
                piece = z[f // 3][ri * 128 : ri * 128 + 128, col : col + 128]
                out[:, at : at + 16, :] = piece.reshape(GY, 16, 128)


def third_kernel(got, th, tl, velocity, vorticity):
    for f in range(6):
        lines = []
        for ri in range(2):
            blocks = []
            for h in range(2):
                at = ((f * 2 + ri) * 2 + h) * 16
                blocks += swap_groups([got[q, at : at + 16, :] for q in range(GY)])
            lines.append(jnp.concatenate(blocks, axis=0))
        u = dot3(split(jnp.concatenate(lines, axis=1)), (th[...], tl[...]))
        out = velocity if f < 3 else vorticity
        out[f % 3] = u.reshape(C1, C2, N3)


def send_lines(force, th, tl, out):
    for f, field in enumerate(force):
        lines = dot3(split(field), (th[...], tl[...]))
        for ri in range(2):
            for h in range(2):
                at = ((f * 2 + ri) * 2 + h) * 16
                v = [
                    lines[(h * 8 + i) * 16 : (h * 8 + i) * 16 + 16, ri * 128 : ri * 128 + 128]
                    for i in range(8)
                ]
                moved = swap_groups(v)
                for q in range(GY):
                    out[q, at : at + 16, :] = moved[q]


def flat_fields(velocity, vorticity):
    return [[part[i].reshape(C1 * C2, N3) for i in range(3)] for part in (velocity, vorticity)]


def force_kernel(velocity, vorticity, th, tl, out):
    u, w = flat_fields(velocity, vorticity)
    send_lines([u[1] * w[2] - u[2] * w[1], u[2] * w[0] - u[0] * w[2]], th, tl, out)


def parted(table):
    return np.concatenate([table[:, 0::2], table[:, 1::2]], axis=1).astype(np.float32).astype(BF)


def rise_tables():
    plain = np.zeros((N3, 2 * N3))
    for i in range(N3):
        plain[i, 2 * i] += 1.0
        for near in (i, (i + 1) % N3):
            plain[near, 2 * i + 1] += 9.0 / 16.0
        for far in ((i - 1) % N3, (i + 2) % N3):
            plain[far, 2 * i + 1] -= 1.0 / 16.0
    face = 0.5 * (plain + np.roll(plain, -1, axis=1))
    return np.stack([parted(plain), parted(face)])


def parity_tables():
    part = parted(np.eye(2 * N3))
    return part, np.ascontiguousarray(part.T)


def three(x):
    high, rest = x.astype(BF), None
    rest = x - high.astype(F32)
    mid = rest.astype(BF)
    return (rest - mid.astype(F32)).astype(BF), mid, high


def permuted(x, table):
    return dots([(part, table) for part in three(x)], ((1,), (0,)))


def middle(a, b, c, d):
    return (9.0 * (b + c) - (a + d)) * (1.0 / 16.0)


def limited(first, second):
    return jnp.maximum(jnp.minimum(second, 0.0), jnp.minimum(first, jnp.maximum(second, 0.0)))


def upwind(face, left, right, jump):
    return face * jnp.where(face > 0.0, left, right) - DIFFUSION_RATIO * jump


def row_divergence(theta, face):
    count = theta.shape[0]
    jump = pltpu.roll(theta, count - 1, 0) - theta
    half = 0.5 * limited(pltpu.roll(jump, 1, 0), jump)
    flux = upwind(face, theta + half, pltpu.roll(theta - half, count - 1, 0), jump)
    return flux - pltpu.roll(flux, 1, 0)


def lane_divergence(even, odd, face_even, face_odd):
    jump_even = odd - even
    jump_odd = pltpu.roll(even, N3 - 1, 1) - odd
    half_even = 0.5 * limited(even - pltpu.roll(odd, 1, 1), jump_even)
    half_odd = 0.5 * limited(jump_even, jump_odd)
    flux_even = upwind(face_even, even + half_even, odd - half_odd, jump_even)
    flux_odd = upwind(face_odd, odd + half_odd, pltpu.roll(even - half_even, N3 - 1, 1), jump_odd)
    return flux_even - pltpu.roll(flux_odd, 1, 1), flux_odd - flux_even


EDGE = 6
SLABS = 2 * C1 + 2 * EDGE
ROWS = 2 * C2 + 16
PTS = C1 + 8
PROWS = C2 + 16


def brick_kernel(scalar, x_low, x_high, y_low, y_high, table, brick, raw):
    raw[0:EDGE, 8:40, :] = x_low[...]
    raw[EDGE : EDGE + 2 * C1, 8:40, :] = scalar[...]
    raw[EDGE + 2 * C1 :, 8:40, :] = x_high[...]
    at = 0
    for layer in range(3):
        first, count = 2 + 2 * layer, 40 - 4 * layer
        raw[first : first + count, 6 - 2 * layer : 8 - 2 * layer, :] = y_low[at : at + count]
        raw[first : first + count, 40 + 2 * layer : 42 + 2 * layer, :] = y_high[at : at + count]
        at += count

    def part(n, carry):
        z = permuted(raw[pl.ds(4 * n, 4)].reshape(4 * ROWS, 256), table[...])
        for h in range(2):
            brick[pl.ds(4 * n, 4), h] = z[:, h * 128 : h * 128 + 128].reshape(4, ROWS, 128)
        return carry

    lax.fori_loop(0, SLABS // 4, part, 0)


def substep(source, target, turn, f1, f2, f3):
    low = 2 + 2 * turn
    begin = []
    for h in range(2):
        t0, t1, t2, t3 = (source[low - 2 + o, h] for o in range(4))
        j0, j1, j2 = t1 - t0, t2 - t1, t3 - t2
        h1, h2 = 0.5 * limited(j0, j1), 0.5 * limited(j1, j2)
        begin.append((t2 + h2, j2, upwind(f1[low - 1, h], t1 + h1, t2 - h2, j1)))

    def step(i, carry):
        here = [source[i, h] for h in range(2)]
        change = list(lane_divergence(*here, f3[i, 0], f3[i, 1]))
        done = []
        for h in range(2):
            left, jump, before = carry[h]
            ahead = source[i + 1, h]
            next_jump = source[i + 2, h] - ahead
            half = 0.5 * limited(jump, next_jump)
            flux = upwind(f1[i, h], left, ahead - half, jump)
            total = change[h] + (flux - before) + row_divergence(here[h], f2[i, h])
            fresh = here[h] - STEP_RATIO * total
            if turn < NSUB - 1:
                target[i, h] = fresh
            else:
                target[i - EDGE, :, h * 128 : h * 128 + 128] = fresh[8:40]
            done.append((ahead + half, next_jump, flux))
        return tuple(done)

    lax.fori_loop(low, SLABS - low, step, tuple(begin))


def early_kernel(
    brick, velocity, vx_low, vx_high, vy_low, vy_high, rise, waited,
    ta, f1, f2, f3,
    vw, su, sf,
):
    for c in range(3):
        vw[c * PTS : c * PTS + 4, 8:24, :] = vx_low[c]
        vw[c * PTS + 4 : c * PTS + 20, 8:24, :] = velocity[c]
        vw[c * PTS + 20 : c * PTS + 24, 8:24, :] = vx_high[c]
        vw[c * PTS : c * PTS + 24, 4:8, :] = vy_low[c]
        vw[c * PTS : c * PTS + 24, 24:28, :] = vy_high[c]
    total = 3 * PTS * PROWS
    for c in range(3):
        table = rise[1 if c == 2 else 0]

        def third(n, carry, c=c, table=table):
            lines = vw[pl.ds(c * PTS + 8 * n, 8)].reshape(8 * PROWS, N3)
            high, low = split(lines)
            z = dots([(low, table), (high, table)], ((1,), (0,)))
            at = pl.multiple_of((c * PTS + 8 * n) * PROWS, 8)
            for h in range(2):
                su[pl.ds(h * total + at, 8 * PROWS), :] = z[:, h * 128 : h * 128 + 128]
            return carry

        lax.fori_loop(0, PTS // 8, third, 0)

    def second(n, carry, c):
        for h in range(2):
            at = pl.multiple_of(h * total + (c * PTS + n) * PROWS, 8)
            p = su[pl.ds(at, PROWS), :]
            a, b, cc, d = (p[4 + o : 25 + o] for o in range(4))
            odd, even = middle(a, b, cc, d), cc
            to = (h * 3 * PTS + c * PTS + n) * ROWS
            if c == 1:
                sf[pl.ds(to + 3, 21, stride=2), :] = 0.5 * (odd + even)
                sf[pl.ds(to + 2, 21, stride=2), :] = 0.5 * (b + odd)
            else:
                sf[pl.ds(to + 3, 21, stride=2), :] = odd
                sf[pl.ds(to + 4, 21, stride=2), :] = even
        return carry

    for c in range(3):
        lax.fori_loop(0, PTS, lambda n, k, c=c: second(n, k, c), 0)

    def first(k, carry):
        for c, face in enumerate((f1, f2, f3)):
            for h in range(2):
                a, b, cc, d = (
                    sf[pl.ds(pl.multiple_of((h * 3 * PTS + c * PTS + k + o) * ROWS, 8), ROWS), :]
                    for o in range(4)
                )
                odd = middle(a, b, cc, d)
                if c == 0:
                    face[2 * k + 1, h] = 0.5 * (odd + cc)
                    face[2 * k, h] = 0.5 * (b + odd)
                else:
                    face[2 * k + 1, h] = odd
                    face[2 * k + 2, h] = cc
        return carry

    lax.fori_loop(0, 21, first, 0)

    substep(brick, ta, 0, f1, f2, f3)


def late_kernel(ta, f1, f2, f3, velocity, vorticity, join, th, tl, waited, advanced, out, tb, last, bs):
    substep(ta, tb, 1, f1, f2, f3)
    substep(tb, last, 2, f1, f2, f3)

    def finish(n, carry):
        lines = last[pl.ds(4 * n, 4)]
        advanced[pl.ds(4 * n, 4)] = permuted(lines.reshape(128, 256), join[...]).reshape(4, 32, 256)
        both = lines[:, :, :128] + lines[:, :, 128:]
        bs[pl.ds(pl.multiple_of(64 * n, 8), 32), :] = 0.125 * (both[0] + both[1])
        bs[pl.ds(pl.multiple_of(64 * n + 32, 8), 32), :] = 0.125 * (both[2] + both[3])
        return carry

    lax.fori_loop(0, C1 // 2, finish, 0)
    buoyancy = bs[pl.ds(0, C1 * C2, stride=2), :] + bs[pl.ds(1, C1 * C2, stride=2), :]
    u, w = flat_fields(velocity, vorticity)
    send_lines([u[0] * w[1] - u[1] * w[0] + buoyancy], th, tl, out)


def second_back_kernel(got, th, tl, out):
    count = got.shape[1] // 64
    columns = []
    for f in range(count):
        for h in range(2):
            parts = []
            for ri in range(2):
                at = ((f * 2 + ri) * 2 + h) * 16
                parts.append(got[:, at : at + 16, :].reshape(128, 128))
            columns.append(jnp.concatenate(parts, axis=0))
    z = dot3((th[...], tl[...]), split(jnp.concatenate(columns, axis=1)))
    for f in range(count):
        for h in range(2):
            at = f * 16 + h * 8
            col = (f * 2 + h) * 128
            out[:, at : at + 8, :] = z[:, col : col + 128].reshape(GX, 8, 128)


def first_back_kernel(got, th, tl, *rest):
    out, y = rest[-2:]
    y[...] = got[...].reshape(N1, 128)
    w = swap_groups([y[pl.ds(g, N1 // 8, stride=8), :] for g in range(8)])
    for i in range(8):
        y[pl.ds(i, N1 // 8, stride=8), :] = w[i]
    z = dot3(split(y[...].T), (th[...], tl[...]))
    for r in range(Q2):
        at = r * 32
        cr, ci = z[at : at + 16, :N1], z[at + 16 : at + 32, :N1]
        sr, si = z[at : at + 16, N1:], z[at + 16 : at + 32, N1:]
        out[0, 0, r] = cr + si
        out[1, 0, r] = ci - sr


def first_back(got, first, start, so_far=None):
    count = got.shape[1] // 16
    whole = pl.BlockSpec(memory_space=pltpu.VMEM)
    args = [got, *first] + ([] if so_far is None else [so_far])
    return pl.pallas_call(
        first_back_kernel,
        grid=(count,),
        out_shape=shape(2, 3, Q2, Q3, N1),
        in_specs=[pl.BlockSpec((GX, 16, 128), lambda f: (0, f, 0)), whole, whole]
        + ([] if so_far is None else [pl.BlockSpec(memory_space=pl.ANY)]),
        out_specs=pl.BlockSpec((2, 1, Q2, Q3, N1), lambda f: (0, f + start, 0, 0, 0)),
        scratch_shapes=[pltpu.VMEM((N1, 128), F32)],
        input_output_aliases={} if so_far is None else {3: 0},
        interpret=INTERPRET,
        name="first_back_kernel",
        compiler_params=pltpu.CompilerParams(vmem_limit_bytes=48 * 1024 * 1024),
    )(*args)


def call(kernel, out_shape, *args, scratch=(), late=0, hbm=None):
    specs = [pl.BlockSpec(memory_space=pltpu.VMEM)] * (len(args) - late)
    specs += [pl.BlockSpec(memory_space=pl.ANY)] * late
    single = not isinstance(out_shape, tuple)
    outs = [out_shape] if single else list(out_shape)
    if hbm is not None:
        outs[int(hbm) if not single else 0] = pltpu.HBM(outs[-1].shape, outs[-1].dtype)
    out_specs = [pl.BlockSpec(memory_space=pltpu.VMEM)] * len(outs)
    return pl.pallas_call(
        kernel,
        in_specs=specs,
        out_specs=out_specs[0] if single else out_specs,
        out_shape=outs[0] if single else outs,
        scratch_shapes=list(scratch),
        interpret=INTERPRET,
        compiler_params=pltpu.CompilerParams(vmem_limit_bytes=48 * 1024 * 1024),
    )(*args)


def shape(*dims):
    return jax.ShapeDtypeStruct(dims, F32)


def ring(axis):
    count = lax.axis_size(axis)
    up = [(i, (i + 1) % count) for i in range(count)]
    return up, [(b, a) for a, b in up]


def edges(axis, first, last):
    up, down = ring(axis)
    low = lax.ppermute(last, axis, up)
    return low, lax.ppermute(first, axis, down)


def exchange(sent, axis):
    return lax.all_to_all(sent, axis, split_axis=0, concat_axis=0, tiled=True)


def step(spectrum, scalar):
    wave_first = np.tile(waves_np(N1).astype(np.float32), 2)[None]
    wave_second = np.repeat(waves_np(N2).astype(np.float32), 2)[:, None]
    blocks = np.tile(waves_np(N3).astype(np.float32).reshape(GY, 1, Q3), (1, 16, 1)).reshape(GY, 1, 256)
    wave_third = lax.dynamic_index_in_dim(jnp.asarray(blocks), lax.axis_index("py"), 0, keepdims=False)
    first = [jnp.asarray(t) for t in first_table()]
    second = [jnp.asarray(t) for t in second_forward()]
    third = [jnp.asarray(t) for t in third_forward()]
    x_low, x_high = edges("px", scalar[:EDGE], scalar[-EDGE:])
    around = jnp.concatenate([x_low[2:], scalar, x_high[:4]], axis=0)
    strips = [
        jnp.concatenate([around[2 * n : 40 - 2 * n, at : at + 2] for n, at in enumerate(starts)], axis=0)
        for starts in ((0, 2, 4), (2 * C2 - 2, 2 * C2 - 4, 2 * C2 - 6))
    ]
    y_low, y_high = edges("py", *strips)
    part, join = (jnp.asarray(t) for t in parity_tables())
    brick = call(
        brick_kernel, shape(SLABS, 2, ROWS, 128), scalar, x_low, x_high, y_low, y_high, part,
        scratch=(pltpu.VMEM((SLABS, ROWS, 256), F32),),
    )
    sent = call(
        first_kernel, shape(GX, 80, 128), spectrum, jnp.asarray(wave_first), *first,
        scratch=(pltpu.VMEM((5 * N1, 128), F32),),
    )
    got = exchange(sent, "px")
    sent = call(second_kernel, shape(GY, 384, 128), got, jnp.asarray(wave_second), wave_third, *second, x_low, x_high, late=2, hbm=True)
    got = exchange(sent, "py")
    velocity, vorticity = call(
        third_kernel, (shape(3, C1, C2, N3), shape(3, C1, C2, N3)), got, *third
    )
    back3 = [jnp.asarray(t) for t in third_back()]
    back2 = [jnp.asarray(t) for t in second_back()]
    sent12 = call(force_kernel, shape(GY, 128, 128), velocity, vorticity, *back3, hbm=True)
    vx_low, vx_high = edges("px", velocity[:, :4], velocity[:, -4:])
    strips = [
        jnp.concatenate([part[:, :, cut] for part in (vx_low, velocity, vx_high)], axis=1)
        for cut in (slice(0, 4), slice(C2 - 4, C2))
    ]
    vy_low, vy_high = edges("py", *strips)
    got12 = exchange(sent12, "py")
    field = shape(SLABS, 2, ROWS, 128)
    once, f1, f2, f3 = call(
        early_kernel, (field, field, field, field),
        brick, velocity, vx_low, vx_high, vy_low, vy_high, jnp.asarray(rise_tables()), sent12,
        scratch=(
            pltpu.VMEM((3 * PTS, PROWS, N3), F32),
            pltpu.VMEM((2 * 3 * PTS * PROWS, 128), F32),
            pltpu.VMEM((2 * 3 * PTS * ROWS, 128), F32),
        ),
        late=1,
    )
    sent12 = call(second_back_kernel, shape(GX, 32, 128), got12, *back2, hbm=True)
    got12 = exchange(sent12, "px")
    theta, sent3 = call(
        late_kernel, (shape(2 * C1, 2 * C2, 2 * N3), shape(GY, 64, 128)),
        once, f1, f2, f3, velocity, vorticity, join, *back3, sent12,
        scratch=(
            pltpu.VMEM((SLABS, 2, ROWS, 128), F32),
            pltpu.VMEM((2 * C1, 2 * C2, 256), F32),
            pltpu.VMEM((2 * C1 * C2, 128), F32),
        ),
        late=1, hbm=1,
    )
    got3 = exchange(sent3, "py")
    sent3 = call(second_back_kernel, shape(GX, 16, 128), got3, *back2, hbm=True)
    got3 = exchange(sent3, "px")
    tendency = first_back(got3, first, 2, first_back(got12, first, 0))
    return tendency, theta


def solution(mesh):
    in_specs = (P(None, None, "px", "py", None), P("px", "py", None))
    out_specs = (P(None, None, "px", "py", None), P("px", "py", None))
    return jax.shard_map(step, mesh=mesh, in_specs=in_specs, out_specs=out_specs, check_vma=False)
```

```python
import math

import jax
import jax.numpy as jnp
import numpy as np
from jax import lax
from jax.experimental import pallas as pl
from jax.experimental.pallas import tpu as pltpu
from jax.sharding import PartitionSpec as P

NSUB = 3
STEP_RATIO = 0.08
DIFFUSION_RATIO = 1.0
INTERPRET = False

N1, N2, N3 = 512, 128, 128
GX, GY = 32, 8
Q2, Q3 = N2 // GX, N3 // GY
C1, C2 = N1 // GX, N2 // GY
FACTOR = 1.0 / math.sqrt(N1 * N2 * N3)
BF = jnp.bfloat16
F32 = jnp.float32


def halves(table):
    high = table.astype(np.float32).astype(BF)
    low = (table - high.astype(np.float64)).astype(np.float32).astype(BF)
    return np.asarray(high), np.asarray(low)


def waves_np(n):
    index = np.arange(n)
    return 2.0 * math.pi / n * np.where(index < n // 2, index, index - n)


def angles(n):
    index = np.arange(n)
    return 2.0 * math.pi / n * (np.outer(index, index) % n)


def first_table():
    a = angles(N1)
    return halves(np.concatenate([np.cos(a), np.sin(a)], axis=1))


def second_forward():
    a = angles(N2)
    plain = np.zeros((2, N2, N2, 2))
    plain[0, :, :, 0] = np.cos(a)
    plain[0, :, :, 1] = -np.sin(a)
    plain[1, :, :, 0] = np.sin(a)
    plain[1, :, :, 1] = np.cos(a)
    turned = np.zeros_like(plain)
    turned[0] = -plain[1]
    turned[1] = plain[0]
    both = np.stack([plain, turned]).reshape(2, 2 * N2, 2 * N2)
    return halves(both)


def third_forward():
    a = angles(N3)
    return halves(FACTOR * np.concatenate([np.cos(a), -np.sin(a)], axis=0))


def third_back():
    a = angles(N3)
    return halves(FACTOR * np.concatenate([np.cos(a), -np.sin(a)], axis=1))


def second_back():
    a = angles(N2)
    table = np.zeros((N2, 2, 2, N2))
    table[:, 0, 0] = np.cos(a)
    table[:, 0, 1] = np.sin(a)
    table[:, 1, 0] = -np.sin(a)
    table[:, 1, 1] = np.cos(a)
    return halves(table.reshape(2 * N2, 2 * N2))


def split(x):
    high = x.astype(BF)
    return high, (x - high.astype(F32)).astype(BF)


def dots(pairs, dims):
    total = None
    for left, right in pairs:
        part = lax.dot_general(left, right, (dims, ((), ())), preferred_element_type=F32)
        total = part if total is None else total + part
    return total


def dot3(left, right, dims=((1,), (0,))):
    lh, ll = left
    rh, rl = right
    return dots([(lh, rl), (ll, rh), (lh, rh)], dims)


def swap_groups(v):
    lane = lax.broadcasted_iota(jnp.int32, v[0].shape, len(v[0].shape) - 1) // 16
    axis = len(v[0].shape) - 1
    v = list(v)
    for s in (1, 2, 4):
        upper = (lane // s) % 2 == 1
        for i in range(8):
            if i & s:
                continue
            a, b = v[i], v[i + s]
            v[i] = jnp.where(upper, pltpu.roll(b, 16 * s, axis), a)
            v[i + s] = jnp.where(upper, b, pltpu.roll(a, 128 - 16 * s, axis))
    return v


def first_kernel(spec, wave, th, tl, out, y):
    rows = []
    for f in (0, 1, 2, 1, 2):
        plain, turned = [], []
        for r in range(Q2):
            re, im = spec[0, f, r], spec[1, f, r]
            plain += [re, im]
            turned += [-im, re]
        piece = jnp.concatenate(
            [jnp.concatenate(plain, axis=0), jnp.concatenate(turned, axis=0)], axis=1
        )
        rows.append(piece if len(rows) < 3 else piece * wave[...])
    table = (th[...], tl[...])
    z = dot3(table, split(jnp.concatenate(rows, axis=0)), ((1,), (1,)))
    for f in range(5):
        y[N1 * f : N1 * f + N1, :] = z[:, 128 * f : 128 * f + 128]
    for f in range(5):
        w = swap_groups([y[pl.ds(N1 * f + i, N1 // 8, stride=8), :] for i in range(8)])
        for g in range(8):
            y[pl.ds(N1 * f + g, N1 // 8, stride=8), :] = w[g]
        out[:, 16 * f : 16 * f + 16, :] = y[N1 * f : N1 * f + N1, :].reshape(GX, 16, 128)


def second_kernel(got, wave2, wave3, th, tl, x_low, x_high, out):
    c = []
    for f in range(5):
        halves_ = [got[:, 16 * f + 8 * h : 16 * f + 8 * h + 8, :].reshape(256, 128) for h in range(2)]
        c.append(jnp.concatenate(halves_, axis=1))
    k2 = wave2[...]
    k3 = wave3[...]
    curl = [k2 * c[2] - k3 * c[1], k3 * c[0] - c[4], c[3] - k2 * c[0]]
    z = []
    for group, fields in enumerate((c[:3], curl)):
        data = split(jnp.concatenate(fields, axis=1))
        z.append(dot3((th[group], tl[group]), data))
    for f in range(6):
        for ri in range(2):
            for h in range(2):
                at = ((f * 2 + ri) * 2 + h) * 16
                col = (f % 3) * 256 + h * 128
                piece = z[f // 3][ri * 128 : ri * 128 + 128, col : col + 128]
                out[:, at : at + 16, :] = piece.reshape(GY, 16, 128)


def third_kernel(got, th, tl, velocity, vorticity):
    for f in range(6):
        lines = []
        for ri in range(2):
            blocks = []
            for h in range(2):
                at = ((f * 2 + ri) * 2 + h) * 16
                blocks += swap_groups([got[q, at : at + 16, :] for q in range(GY)])
            lines.append(jnp.concatenate(blocks, axis=0))
        u = dot3(split(jnp.concatenate(lines, axis=1)), (th[...], tl[...]))
        out = velocity if f < 3 else vorticity
        out[f % 3] = u.reshape(C1, C2, N3)


def force_lines(velocity, vorticity, b, th, tl, out):
    u = [velocity[i].reshape(C1 * C2, N3) for i in range(3)]
    w = [vorticity[i].reshape(C1 * C2, N3) for i in range(3)]
    force = [u[1] * w[2] - u[2] * w[1], u[2] * w[0] - u[0] * w[2], u[0] * w[1] - u[1] * w[0] + b]
    for f in range(3):
        lines = dot3(split(force[f]), (th[...], tl[...]))
        for ri in range(2):
            for h in range(2):
                at = ((f * 2 + ri) * 2 + h) * 16
                v = [
                    lines[(h * 8 + i) * 16 : (h * 8 + i) * 16 + 16, ri * 128 : ri * 128 + 128]
                    for i in range(8)
                ]
                w8 = swap_groups(v)
                for q in range(GY):
                    out[q, at : at + 16, :] = w8[q]


def parted(table):
    return np.concatenate([table[:, 0::2], table[:, 1::2]], axis=1).astype(np.float32).astype(BF)


def rise_tables():
    plain = np.zeros((N3, 2 * N3))
    for i in range(N3):
        plain[i, 2 * i] += 1.0
        for near in (i, (i + 1) % N3):
            plain[near, 2 * i + 1] += 9.0 / 16.0
        for far in ((i - 1) % N3, (i + 2) % N3):
            plain[far, 2 * i + 1] -= 1.0 / 16.0
    face = 0.5 * (plain + np.roll(plain, -1, axis=1))
    return np.stack([parted(plain), parted(face)])


def parity_tables():
    part = parted(np.eye(2 * N3))
    return part, np.ascontiguousarray(part.T)


def three(x):
    high, rest = x.astype(BF), None
    rest = x - high.astype(F32)
    mid = rest.astype(BF)
    return (rest - mid.astype(F32)).astype(BF), mid, high


def permuted(x, table):
    return dots([(part, table) for part in three(x)], ((1,), (0,)))


def middle(a, b, c, d):
    return (9.0 * (b + c) - (a + d)) * (1.0 / 16.0)


def limited(first, second):
    return jnp.maximum(jnp.minimum(second, 0.0), jnp.minimum(first, jnp.maximum(second, 0.0)))


def upwind(face, left, right, jump):
    return face * jnp.where(face > 0.0, left, right) - DIFFUSION_RATIO * jump


def row_divergence(theta, face):
    count = theta.shape[0]
    jump = pltpu.roll(theta, count - 1, 0) - theta
    half = 0.5 * limited(pltpu.roll(jump, 1, 0), jump)
    flux = upwind(face, theta + half, pltpu.roll(theta - half, count - 1, 0), jump)
    return flux - pltpu.roll(flux, 1, 0)


def lane_divergence(even, odd, face_even, face_odd, face_before):
    even_before, odd_before = pltpu.roll(even, 1, 1), pltpu.roll(odd, 1, 1)
    even_after, odd_after = pltpu.roll(even, N3 - 1, 1), pltpu.roll(odd, N3 - 1, 1)
    jump_even = odd - even
    jump_odd = even_after - odd
    jump_before = even - odd_before
    half_even = 0.5 * limited(jump_before, jump_even)
    half_odd = 0.5 * limited(jump_even, jump_odd)
    half_before = 0.5 * limited(odd_before - even_before, jump_before)
    half_after = 0.5 * limited(jump_odd, odd_after - even_after)
    flux_even = upwind(face_even, even + half_even, odd - half_odd, jump_even)
    flux_odd = upwind(face_odd, odd + half_odd, even_after - half_after, jump_odd)
    flux_before = upwind(face_before, odd_before + half_before, even - half_even, jump_before)
    return flux_even - flux_before, flux_odd - flux_even


EDGE = 6
SLABS = 2 * C1 + 2 * EDGE
ROWS = 2 * C2 + 16
PTS = C1 + 8
PROWS = C2 + 16


def brick_kernel(scalar, x_low, x_high, y_low, y_high, table, brick, raw):
    raw[0:EDGE, 8:40, :] = x_low[...]
    raw[EDGE : EDGE + 2 * C1, 8:40, :] = scalar[...]
    raw[EDGE + 2 * C1 :, 8:40, :] = x_high[...]
    at = 0
    for layer in range(3):
        first, count = 2 + 2 * layer, 40 - 4 * layer
        raw[first : first + count, 6 - 2 * layer : 8 - 2 * layer, :] = y_low[at : at + count]
        raw[first : first + count, 40 + 2 * layer : 42 + 2 * layer, :] = y_high[at : at + count]
        at += count

    def part(n, carry):
        z = permuted(raw[pl.ds(4 * n, 4)].reshape(4 * ROWS, 256), table[...])
        for h in range(2):
            brick[pl.ds(4 * n, 4), h] = z[:, h * 128 : h * 128 + 128].reshape(4, ROWS, 128)
        return carry

    lax.fori_loop(0, SLABS // 4, part, 0)


def scalar_kernel(
    brick, velocity, vx_low, vx_high, vy_low, vy_high, vorticity,
    rise, join, th, tl,
    advanced, out,
    ta, tb, last, vw, su, sf, f1, f2, f3, bs,
):
    for c in range(3):
        vw[c * PTS : c * PTS + 4, 8:24, :] = vx_low[c]
        vw[c * PTS + 4 : c * PTS + 20, 8:24, :] = velocity[c]
        vw[c * PTS + 20 : c * PTS + 24, 8:24, :] = vx_high[c]
        vw[c * PTS : c * PTS + 24, 4:8, :] = vy_low[c]
        vw[c * PTS : c * PTS + 24, 24:28, :] = vy_high[c]
    total = 3 * PTS * PROWS
    for c in range(3):
        table = rise[1 if c == 2 else 0]

        def third(n, carry, c=c, table=table):
            lines = vw[pl.ds(c * PTS + 8 * n, 8)].reshape(8 * PROWS, N3)
            high, low = split(lines)
            z = dots([(low, table), (high, table)], ((1,), (0,)))
            at = pl.multiple_of((c * PTS + 8 * n) * PROWS, 8)
            for h in range(2):
                su[pl.ds(h * total + at, 8 * PROWS), :] = z[:, h * 128 : h * 128 + 128]
            return carry

        lax.fori_loop(0, PTS // 8, third, 0)

    def second(n, carry, c):
        for h in range(2):
            at = pl.multiple_of(h * total + (c * PTS + n) * PROWS, 8)
            p = su[pl.ds(at, PROWS), :]
            a, b, cc, d = (p[4 + o : 25 + o] for o in range(4))
            odd, even = middle(a, b, cc, d), cc
            to = (h * 3 * PTS + c * PTS + n) * ROWS
            if c == 1:
                sf[pl.ds(to + 3, 21, stride=2), :] = 0.5 * (odd + even)
                sf[pl.ds(to + 2, 21, stride=2), :] = 0.5 * (b + odd)
            else:
                sf[pl.ds(to + 3, 21, stride=2), :] = odd
                sf[pl.ds(to + 4, 21, stride=2), :] = even
        return carry

    for c in range(3):
        lax.fori_loop(0, PTS, lambda n, k, c=c: second(n, k, c), 0)

    def first(k, carry):
        for c, face in enumerate((f1, f2, f3)):
            for h in range(2):
                a, b, cc, d = (
                    sf[pl.ds(pl.multiple_of((h * 3 * PTS + c * PTS + k + o) * ROWS, 8), ROWS), :]
                    for o in range(4)
                )
                odd = middle(a, b, cc, d)
                if c == 0:
                    face[2 * k + 1, h] = 0.5 * (odd + cc)
                    face[2 * k, h] = 0.5 * (b + odd)
                else:
                    face[2 * k + 1, h] = odd
                    face[2 * k + 2, h] = cc
                if c == 2 and h == 1:
                    face[2 * k + 1, 2] = pltpu.roll(odd, 1, 1)
                    face[2 * k + 2, 2] = pltpu.roll(cc, 1, 1)
        return carry

    lax.fori_loop(0, 21, first, 0)

    for turn, (source, target) in enumerate(((brick, ta), (ta, tb), (tb, last))):
        low = 2 + 2 * turn
        begin = []
        for h in range(2):
            t0, t1, t2, t3 = (source[low - 2 + o, h] for o in range(4))
            j0, j1, j2 = t1 - t0, t2 - t1, t3 - t2
            h1, h2 = 0.5 * limited(j0, j1), 0.5 * limited(j1, j2)
            begin.append((t2 + h2, j2, upwind(f1[low - 1, h], t1 + h1, t2 - h2, j1)))

        def step(i, carry, source=source, target=target, turn=turn):
            here = [source[i, h] for h in range(2)]
            change = list(lane_divergence(*here, f3[i, 0], f3[i, 1], f3[i, 2]))
            done = []
            for h in range(2):
                left, jump, before = carry[h]
                ahead = source[i + 1, h]
                next_jump = source[i + 2, h] - ahead
                half = 0.5 * limited(jump, next_jump)
                flux = upwind(f1[i, h], left, ahead - half, jump)
                total = change[h] + (flux - before) + row_divergence(here[h], f2[i, h])
                fresh = here[h] - STEP_RATIO * total
                if turn < NSUB - 1:
                    target[i, h] = fresh
                else:
                    target[i - EDGE, :, h * 128 : h * 128 + 128] = fresh[8:40]
                done.append((ahead + half, next_jump, flux))
            return tuple(done)

        lax.fori_loop(low, SLABS - low, step, tuple(begin))

    def finish(n, carry):
        lines = last[pl.ds(4 * n, 4)]
        advanced[pl.ds(4 * n, 4)] = permuted(lines.reshape(128, 256), join[...]).reshape(4, 32, 256)
        both = lines[:, :, :128] + lines[:, :, 128:]
        bs[pl.ds(pl.multiple_of(64 * n, 8), 32), :] = 0.125 * (both[0] + both[1])
        bs[pl.ds(pl.multiple_of(64 * n + 32, 8), 32), :] = 0.125 * (both[2] + both[3])
        return carry

    lax.fori_loop(0, C1 // 2, finish, 0)
    buoyancy = bs[pl.ds(0, C1 * C2, stride=2), :] + bs[pl.ds(1, C1 * C2, stride=2), :]
    force_lines(velocity, vorticity, buoyancy, th, tl, out)


def second_back_kernel(got, th, tl, out):
    columns = []
    for f in range(3):
        for h in range(2):
            parts = []
            for ri in range(2):
                at = ((f * 2 + ri) * 2 + h) * 16
                parts.append(got[:, at : at + 16, :].reshape(128, 128))
            columns.append(jnp.concatenate(parts, axis=0))
    z = dot3((th[...], tl[...]), split(jnp.concatenate(columns, axis=1)))
    for f in range(3):
        for h in range(2):
            at = f * 16 + h * 8
            col = (f * 2 + h) * 128
            out[:, at : at + 8, :] = z[:, col : col + 128].reshape(GX, 8, 128)


def first_back_kernel(got, th, tl, out, y):
    rows = []
    for f in range(3):
        y[...] = got[:, 16 * f : 16 * f + 16, :].reshape(N1, 128)
        w = swap_groups([y[pl.ds(g, N1 // 8, stride=8), :] for g in range(8)])
        for i in range(8):
            y[pl.ds(i, N1 // 8, stride=8), :] = w[i]
        rows.append(y[...].T)
    z = dot3(split(jnp.concatenate(rows, axis=0)), (th[...], tl[...]))
    for f in range(3):
        for r in range(Q2):
            at = f * 128 + r * 32
            cr, ci = z[at : at + 16, :N1], z[at + 16 : at + 32, :N1]
            sr, si = z[at : at + 16, N1:], z[at + 16 : at + 32, N1:]
            out[0, f, r] = cr + si
            out[1, f, r] = ci - sr


def call(kernel, out_shape, *args, scratch=(), late=0, hbm=False):
    specs = [pl.BlockSpec(memory_space=pltpu.VMEM)] * (len(args) - late)
    specs += [pl.BlockSpec(memory_space=pl.ANY)] * late
    return pl.pallas_call(
        kernel,
        in_specs=specs,
        out_shape=out_shape if not hbm else pltpu.HBM(out_shape.shape, out_shape.dtype),
        out_specs=jax.tree.map(lambda _: pl.BlockSpec(memory_space=pltpu.VMEM), out_shape),
        scratch_shapes=list(scratch),
        interpret=INTERPRET,
        name=kernel.__name__,
        compiler_params=pltpu.CompilerParams(vmem_limit_bytes=48 * 1024 * 1024),
    )(*args)


def shape(*dims):
    return jax.ShapeDtypeStruct(dims, F32)


def ring(axis):
    count = lax.axis_size(axis)
    up = [(i, (i + 1) % count) for i in range(count)]
    return up, [(b, a) for a, b in up]


def edges(axis, first, last):
    up, down = ring(axis)
    return lax.ppermute(last, axis, up), lax.ppermute(first, axis, down)


def body(spectrum, scalar):
    wave_first = np.tile(waves_np(N1).astype(np.float32), 2)[None]
    wave_second = np.repeat(waves_np(N2).astype(np.float32), 2)[:, None]
    blocks = np.tile(waves_np(N3).astype(np.float32).reshape(GY, 1, Q3), (1, 16, 1)).reshape(GY, 1, 256)
    wave_third = lax.dynamic_index_in_dim(jnp.asarray(blocks), lax.axis_index("py"), 0, keepdims=False)
    first = [jnp.asarray(t) for t in first_table()]
    second = [jnp.asarray(t) for t in second_forward()]
    third = [jnp.asarray(t) for t in third_forward()]
    x_low, x_high = edges("px", scalar[:EDGE], scalar[-EDGE:])
    around = jnp.concatenate([x_low[2:], scalar, x_high[:4]], axis=0)
    strips = [
        jnp.concatenate([around[2 * n : 40 - 2 * n, at : at + 2] for n, at in enumerate(starts)], axis=0)
        for starts in ((0, 2, 4), (2 * C2 - 2, 2 * C2 - 4, 2 * C2 - 6))
    ]
    y_low, y_high = edges("py", *strips)
    part, join = (jnp.asarray(t) for t in parity_tables())
    brick = call(
        brick_kernel, shape(SLABS, 2, ROWS, 128), scalar, x_low, x_high, y_low, y_high, part,
        scratch=(pltpu.VMEM((SLABS, ROWS, 256), F32),),
    )
    sent = call(
        first_kernel, shape(GX, 80, 128), spectrum, jnp.asarray(wave_first), *first,
        scratch=(pltpu.VMEM((5 * N1, 128), F32),),
    )
    got = lax.all_to_all(sent, "px", split_axis=0, concat_axis=0, tiled=True)
    sent = call(second_kernel, shape(GY, 384, 128), got, jnp.asarray(wave_second), wave_third, *second, x_low, x_high, late=2, hbm=True)
    got = lax.all_to_all(sent, "py", split_axis=0, concat_axis=0, tiled=True)
    velocity, vorticity = call(
        third_kernel, (shape(3, C1, C2, N3), shape(3, C1, C2, N3)), got, *third
    )
    vx_low, vx_high = edges("px", velocity[:, :4], velocity[:, -4:])
    strips = [
        jnp.concatenate([part[:, :, cut] for part in (vx_low, velocity, vx_high)], axis=1)
        for cut in (slice(0, 4), slice(C2 - 4, C2))
    ]
    vy_low, vy_high = edges("py", *strips)
    theta, sent = call(
        scalar_kernel, (shape(2 * C1, 2 * C2, 2 * N3), shape(GY, 192, 128)),
        brick, velocity, vx_low, vx_high, vy_low, vy_high, vorticity,
        jnp.asarray(rise_tables()), join, *[jnp.asarray(t) for t in third_back()],
        scratch=(
            pltpu.VMEM((SLABS, 2, ROWS, 128), F32),
            pltpu.VMEM((SLABS, 2, ROWS, 128), F32),
            pltpu.VMEM((2 * C1, 2 * C2, 256), F32),
            pltpu.VMEM((3 * PTS, PROWS, N3), F32),
            pltpu.VMEM((2 * 3 * PTS * PROWS, 128), F32),
            pltpu.VMEM((2 * 3 * PTS * ROWS, 128), F32),
            pltpu.VMEM((SLABS, 2, ROWS, 128), F32),
            pltpu.VMEM((SLABS, 2, ROWS, 128), F32),
            pltpu.VMEM((SLABS, 3, ROWS, 128), F32),
            pltpu.VMEM((2 * C1 * C2, 128), F32),
        ),
    )
    got = lax.all_to_all(sent, "py", split_axis=0, concat_axis=0, tiled=True)
    sent = call(
        second_back_kernel, shape(GX, 48, 128), got, *[jnp.asarray(t) for t in second_back()]
    )
    got = lax.all_to_all(sent, "px", split_axis=0, concat_axis=0, tiled=True)
    tendency = call(
        first_back_kernel, shape(2, 3, Q2, Q3, N1), got, *first,
        scratch=(pltpu.VMEM((N1, 128), F32),),
    )
    return tendency, theta


def solution(mesh):
    in_specs = (P(None, None, "px", "py", None), P("px", "py", None))
    out_specs = (P(None, None, "px", "py", None), P("px", "py", None))
    return jax.shard_map(body, mesh=mesh, in_specs=in_specs, out_specs=out_specs, check_vma=False)
```

```python
import math

import jax
import jax.numpy as jnp
import numpy as np
from jax import lax
from jax.experimental import pallas as pl
from jax.experimental.pallas import tpu as pltpu
from jax.sharding import PartitionSpec as P

NSUB = 3
STEP_RATIO = 0.08
DIFFUSION_RATIO = 1.0
INTERPRET = False

N1, N2, N3 = 512, 128, 128
GX, GY = 32, 8
Q2, Q3 = N2 // GX, N3 // GY
C1, C2 = N1 // GX, N2 // GY
FACTOR = 1.0 / math.sqrt(N1 * N2 * N3)
BF = jnp.bfloat16
F32 = jnp.float32


def halves(table):
    high = table.astype(np.float32).astype(BF)
    low = (table - high.astype(np.float64)).astype(np.float32).astype(BF)
    return np.asarray(high), np.asarray(low)


def waves_np(n):
    index = np.arange(n)
    return 2.0 * math.pi / n * np.where(index < n // 2, index, index - n)


def angles(n):
    index = np.arange(n)
    return 2.0 * math.pi / n * (np.outer(index, index) % n)


def first_table():
    a = angles(N1)[:, : N1 // 2]
    rows = np.concatenate([a[0::2], a[1::2]], axis=0)
    return halves(np.concatenate([np.cos(rows), np.sin(rows)], axis=1))


def second_forward():
    a = angles(N2)
    table = np.zeros((2, N2, N2, 2))
    table[0, :, :, 0] = np.cos(a)
    table[0, :, :, 1] = -np.sin(a)
    table[1, :, :, 0] = np.sin(a)
    table[1, :, :, 1] = np.cos(a)
    return halves(table.reshape(2 * N2, 2 * N2))


def third_forward():
    a = angles(N3)
    return halves(FACTOR * np.concatenate([np.cos(a), -np.sin(a)], axis=0))


def split(x):
    high = x.astype(BF)
    return high, (x - high.astype(F32)).astype(BF)


def dots(pairs, dims):
    total = None
    for left, right in pairs:
        part = lax.dot_general(left, right, (dims, ((), ())), preferred_element_type=F32)
        total = part if total is None else total + part
    return total


def dot3(left, right, dims=((1,), (0,))):
    lh, ll = left
    rh, rl = right
    return dots([(lh, rl), (ll, rh), (lh, rh)], dims)


def swap_groups(v):
    lane = lax.broadcasted_iota(jnp.int32, v[0].shape, len(v[0].shape) - 1) // 16
    axis = len(v[0].shape) - 1
    v = list(v)
    for s in (1, 2, 4):
        upper = (lane // s) % 2 == 1
        for i in range(8):
            if i & s:
                continue
            a, b = v[i], v[i + s]
            v[i] = jnp.where(upper, pltpu.roll(b, 16 * s, axis), a)
            v[i + s] = jnp.where(upper, b, pltpu.roll(a, 128 - 16 * s, axis))
    return v


HALF = N1 // 2


def point_row(i):
    return HALF * (i % 2) + i // 2


def first_kernel(spec, wave, th, tl, out, y):
    even, odd = [], []
    for n, f in enumerate((0, 1, 2, 1, 2)):
        plain, turned = [], []
        for r in range(Q2):
            re, im = spec[0, f, r], spec[1, f, r]
            if n > 2:
                re, im = re * wave[...], im * wave[...]
            plain += [re, im]
            turned += [-im, re]
        pieces = [jnp.concatenate(part, axis=0) for part in (plain, turned)]
        even.append(jnp.concatenate([p[:, :HALF] + p[:, HALF:] for p in pieces], axis=1))
        odd.append(jnp.concatenate([p[:, :HALF] - p[:, HALF:] for p in pieces], axis=1))
    for n, rows in enumerate((even, odd)):
        table = (th[HALF * n : HALF * n + HALF, :], tl[HALF * n : HALF * n + HALF, :])
        z = dot3(table, split(jnp.concatenate(rows, axis=0)), ((1,), (1,)))
        for f in range(5):
            at = N1 * f + HALF * n
            y[at : at + HALF, :] = z[:, 128 * f : 128 * f + 128]
    for f in range(5):
        w = swap_groups([y[pl.ds(N1 * f + point_row(i), N1 // 8, stride=4), :] for i in range(8)])
        for g in range(8):
            y[pl.ds(N1 * f + g, N1 // 8, stride=8), :] = w[g]
        out[:, 16 * f : 16 * f + 16, :] = y[N1 * f : N1 * f + N1, :].reshape(GX, 16, 128)


def second_kernel(got, wave2, wave3, th, tl, x_low, x_high, out):
    c = []
    for f in range(5):
        halves_ = [got[:, 16 * f + 8 * h : 16 * f + 8 * h + 8, :].reshape(256, 128) for h in range(2)]
        c.append(jnp.concatenate(halves_, axis=1))
    k2 = wave2[...]
    k3 = wave3[...]
    curl = [k2 * c[2] - k3 * c[1], k3 * c[0] - c[4], c[3] - k2 * c[0]]
    z = dot3((th[...], tl[...]), split(jnp.concatenate(c[:3] + curl, axis=1)))
    for f in range(6):
        real = z[:128, 256 * f : 256 * f + 256]
        imag = z[128:, 256 * f : 256 * f + 256]
        for ri, part in enumerate((real, imag) if f < 3 else (-imag, real)):
            for h in range(2):
                at = ((f * 2 + ri) * 2 + h) * 16
                out[:, at : at + 16, :] = part[:, h * 128 : h * 128 + 128].reshape(GY, 16, 128)


def third_kernel(got, th, tl, velocity, vorticity):
    for f in range(6):
        lines = []
        for ri in range(2):
            blocks = []
            for h in range(2):
                at = ((f * 2 + ri) * 2 + h) * 16
                blocks += swap_groups([got[q, at : at + 16, :] for q in range(GY)])
            lines.append(jnp.concatenate(blocks, axis=0))
        u = dot3(split(jnp.concatenate(lines, axis=1)), (th[...], tl[...]))
        out = velocity if f < 3 else vorticity
        out[f % 3] = u.reshape(C1, C2, N3)


def force_lines(velocity, vorticity, b, th, tl, out):
    u = [velocity[i].reshape(C1 * C2, N3) for i in range(3)]
    w = [vorticity[i].reshape(C1 * C2, N3) for i in range(3)]
    force = [u[1] * w[2] - u[2] * w[1], u[2] * w[0] - u[0] * w[2], u[0] * w[1] - u[1] * w[0] + b]
    for f in range(3):
        lines = dot3(split(force[f]), (th[...], tl[...]), ((1,), (1,)))
        for ri in range(2):
            for h in range(2):
                at = ((f * 2 + ri) * 2 + h) * 16
                v = [
                    lines[(h * 8 + i) * 16 : (h * 8 + i) * 16 + 16, ri * 128 : ri * 128 + 128]
                    for i in range(8)
                ]
                w8 = swap_groups(v)
                for q in range(GY):
                    out[q, at : at + 16, :] = w8[q]


def parted(table):
    return np.concatenate([table[:, 0::2], table[:, 1::2]], axis=1).astype(np.float32).astype(BF)


def rise_tables():
    plain = np.zeros((N3, 2 * N3))
    for i in range(N3):
        plain[i, 2 * i] += 1.0
        for near in (i, (i + 1) % N3):
            plain[near, 2 * i + 1] += 9.0 / 16.0
        for far in ((i - 1) % N3, (i + 2) % N3):
            plain[far, 2 * i + 1] -= 1.0 / 16.0
    face = 0.5 * (plain + np.roll(plain, -1, axis=1))
    return np.stack([parted(plain), parted(face)])


def parity_table():
    return parted(np.eye(2 * N3))


def three(x):
    high, rest = x.astype(BF), None
    rest = x - high.astype(F32)
    mid = rest.astype(BF)
    return (rest - mid.astype(F32)).astype(BF), mid, high


def permuted(x, table, dims=((1,), (0,))):
    return dots([(part, table) for part in three(x)], dims)


def middle(a, b, c, d):
    return (9.0 * (b + c) - (a + d)) * (1.0 / 16.0)


def limited(first, second):
    return jnp.maximum(jnp.minimum(second, 0.0), jnp.minimum(first, jnp.maximum(second, 0.0)))


def upwind(face, left, right, jump):
    return face * jnp.where(face > 0.0, left, right) - DIFFUSION_RATIO * jump


def row_divergence(theta, face):
    count = theta.shape[0]
    jump = pltpu.roll(theta, count - 1, 0) - theta
    half = 0.5 * limited(pltpu.roll(jump, 1, 0), jump)
    flux = upwind(face, theta + half, pltpu.roll(theta - half, count - 1, 0), jump)
    return flux - pltpu.roll(flux, 1, 0)


def lane_divergence(even, odd, face_even, face_odd, face_before):
    even_before, odd_before = pltpu.roll(even, 1, 1), pltpu.roll(odd, 1, 1)
    even_after, odd_after = pltpu.roll(even, N3 - 1, 1), pltpu.roll(odd, N3 - 1, 1)
    jump_even = odd - even
    jump_odd = even_after - odd
    jump_before = even - odd_before
    half_even = 0.5 * limited(jump_before, jump_even)
    half_odd = 0.5 * limited(jump_even, jump_odd)
    half_before = 0.5 * limited(odd_before - even_before, jump_before)
    half_after = 0.5 * limited(jump_odd, odd_after - even_after)
    flux_even = upwind(face_even, even + half_even, odd - half_odd, jump_even)
    flux_odd = upwind(face_odd, odd + half_odd, even_after - half_after, jump_odd)
    flux_before = upwind(face_before, odd_before + half_before, even - half_even, jump_before)
    return flux_even - flux_before, flux_odd - flux_even


EDGE = 6
SLABS = 2 * C1 + 2 * EDGE
ROWS = 2 * C2 + 16
PTS = C1 + 8
PROWS = C2 + 16


def brick_kernel(scalar, x_low, x_high, y_low, y_high, table, brick, raw):
    raw[0:EDGE, 8:40, :] = x_low[...]
    raw[EDGE : EDGE + 2 * C1, 8:40, :] = scalar[...]
    raw[EDGE + 2 * C1 :, 8:40, :] = x_high[...]
    at = 0
    for layer in range(3):
        first, count = 2 + 2 * layer, 40 - 4 * layer
        raw[first : first + count, 6 - 2 * layer : 8 - 2 * layer, :] = y_low[at : at + count]
        raw[first : first + count, 40 + 2 * layer : 42 + 2 * layer, :] = y_high[at : at + count]
        at += count

    def sort(n, carry):
        z = permuted(raw[pl.ds(4 * n, 4)].reshape(4 * ROWS, 256), table[...])
        for h in range(2):
            brick[pl.ds(4 * n, 4), h] = z[:, h * 128 : h * 128 + 128].reshape(4, ROWS, 128)
        return carry

    lax.fori_loop(0, SLABS // 4, sort, 0)


def scalar_kernel(
    brick, velocity, vx_low, vx_high, vy_low, vy_high, vorticity,
    rise, part, th, tl,
    advanced, out,
    ta, tb, last, vw, su, sf, f1, f2, f3, bs,
):
    for c in range(3):
        vw[c * PTS : c * PTS + 4, 8:24, :] = vx_low[c]
        vw[c * PTS + 4 : c * PTS + 20, 8:24, :] = velocity[c]
        vw[c * PTS + 20 : c * PTS + 24, 8:24, :] = vx_high[c]
        vw[c * PTS : c * PTS + 24, 4:8, :] = vy_low[c]
        vw[c * PTS : c * PTS + 24, 24:28, :] = vy_high[c]
    total = 3 * PTS * PROWS
    for c in range(3):
        table = rise[1 if c == 2 else 0]

        def third(n, carry, c=c, table=table):
            lines = vw[pl.ds(c * PTS + 8 * n, 8)].reshape(8 * PROWS, N3)
            high, low = split(lines)
            z = dots([(low, table), (high, table)], ((1,), (0,)))
            at = pl.multiple_of((c * PTS + 8 * n) * PROWS, 8)
            for h in range(2):
                su[pl.ds(h * total + at, 8 * PROWS), :] = z[:, h * 128 : h * 128 + 128]
            return carry

        lax.fori_loop(0, PTS // 8, third, 0)

    def second(n, carry, c):
        for h in range(2):
            at = pl.multiple_of(h * total + (c * PTS + n) * PROWS, 8)
            p = su[pl.ds(at, PROWS), :]
            a, b, cc, d = (p[4 + o : 25 + o] for o in range(4))
            odd, even = middle(a, b, cc, d), cc
            to = (h * 3 * PTS + c * PTS + n) * ROWS
            if c == 1:
                sf[pl.ds(to + 3, 21, stride=2), :] = 0.5 * (odd + even)
                sf[pl.ds(to + 2, 21, stride=2), :] = 0.5 * (b + odd)
            else:
                sf[pl.ds(to + 3, 21, stride=2), :] = odd
                sf[pl.ds(to + 4, 21, stride=2), :] = even
        return carry

    for c in range(3):
        lax.fori_loop(0, PTS, lambda n, k, c=c: second(n, k, c), 0)

    def first(k, carry):
        for c, face in enumerate((f1, f2, f3)):
            for h in range(2):
                a, b, cc, d = (
                    sf[pl.ds(pl.multiple_of((h * 3 * PTS + c * PTS + k + o) * ROWS, 8), ROWS), :]
                    for o in range(4)
                )
                odd = middle(a, b, cc, d)
                if c == 0:
                    face[2 * k + 1, h] = 0.5 * (odd + cc)
                    face[2 * k, h] = 0.5 * (b + odd)
                else:
                    face[2 * k + 1, h] = odd
                    face[2 * k + 2, h] = cc
                if c == 2 and h == 1:
                    face[2 * k + 1, 2] = pltpu.roll(odd, 1, 1)
                    face[2 * k + 2, 2] = pltpu.roll(cc, 1, 1)
        return carry

    lax.fori_loop(0, 21, first, 0)

    for turn, (source, target) in enumerate(((brick, ta), (ta, tb), (tb, last))):
        low = 2 + 2 * turn
        begin = []
        for h in range(2):
            t0, t1, t2, t3 = (source[low - 2 + o, h] for o in range(4))
            j0, j1, j2 = t1 - t0, t2 - t1, t3 - t2
            h1, h2 = 0.5 * limited(j0, j1), 0.5 * limited(j1, j2)
            begin.append((t2 + h2, j2, upwind(f1[low - 1, h], t1 + h1, t2 - h2, j1)))

        def step(i, carry, source=source, target=target, turn=turn):
            here = [source[i, h] for h in range(2)]
            change = list(lane_divergence(*here, f3[i, 0], f3[i, 1], f3[i, 2]))
            done = []
            for h in range(2):
                left, jump, before = carry[h]
                ahead = source[i + 1, h]
                next_jump = source[i + 2, h] - ahead
                half = 0.5 * limited(jump, next_jump)
                flux = upwind(f1[i, h], left, ahead - half, jump)
                total = change[h] + (flux - before) + row_divergence(here[h], f2[i, h])
                fresh = here[h] - STEP_RATIO * total
                if turn < NSUB - 1:
                    target[i, h] = fresh
                else:
                    target[i - EDGE, :, h * 128 : h * 128 + 128] = fresh[8:40]
                done.append((ahead + half, next_jump, flux))
            return tuple(done)

        lax.fori_loop(low, SLABS - low, step, tuple(begin))

    def finish(n, carry):
        lines = last[pl.ds(4 * n, 4)]
        advanced[pl.ds(4 * n, 4)] = permuted(lines.reshape(128, 256), part[...], ((1,), (1,))).reshape(4, 32, 256)
        both = lines[:, :, :128] + lines[:, :, 128:]
        bs[pl.ds(pl.multiple_of(64 * n, 8), 32), :] = 0.125 * (both[0] + both[1])
        bs[pl.ds(pl.multiple_of(64 * n + 32, 8), 32), :] = 0.125 * (both[2] + both[3])
        return carry

    lax.fori_loop(0, C1 // 2, finish, 0)
    buoyancy = bs[pl.ds(0, C1 * C2, stride=2), :] + bs[pl.ds(1, C1 * C2, stride=2), :]
    force_lines(velocity, vorticity, buoyancy, th, tl, out)


def second_back_kernel(got, th, tl, out):
    columns = []
    for f in range(3):
        for h in range(2):
            parts = []
            for ri in range(2):
                at = ((f * 2 + ri) * 2 + h) * 16
                parts.append(got[:, at : at + 16, :].reshape(128, 128))
            columns.append(jnp.concatenate(parts, axis=0))
    z = dot3((th[...], tl[...]), split(jnp.concatenate(columns, axis=1)), ((0,), (0,)))
    for f in range(3):
        for h in range(2):
            at = f * 16 + h * 8
            col = (f * 2 + h) * 128
            out[:, at : at + 8, :] = z[:, col : col + 128].reshape(GX, 8, 128)


def first_back_kernel(got, th, tl, out, y):
    rows = ([], [])
    for f in range(3):
        y[...] = got[:, 16 * f : 16 * f + 16, :].reshape(N1, 128)
        w = swap_groups([y[pl.ds(g, N1 // 8, stride=8), :] for g in range(8)])
        for i in range(8):
            y[pl.ds(point_row(i), N1 // 8, stride=4), :] = w[i]
        for n in range(2):
            rows[n].append(y[HALF * n : HALF * n + HALF, :].T)
    z = []
    for n in range(2):
        table = (th[HALF * n : HALF * n + HALF, :], tl[HALF * n : HALF * n + HALF, :])
        z.append(dot3(split(jnp.concatenate(rows[n], axis=0)), table))
    for f in range(3):
        for r in range(Q2):
            at = f * 128 + r * 32
            real = [p[at : at + 16, :HALF] + p[at + 16 : at + 32, HALF:] for p in z]
            imag = [p[at + 16 : at + 32, :HALF] - p[at : at + 16, HALF:] for p in z]
            for ri, (e, o) in enumerate((real, imag)):
                out[ri, f, r] = jnp.concatenate([e + o, e - o], axis=1)


def call(kernel, out_shape, *args, scratch=(), late=0, hbm=False):
    specs = [pl.BlockSpec(memory_space=pltpu.VMEM)] * (len(args) - late)
    specs += [pl.BlockSpec(memory_space=pl.ANY)] * late
    return pl.pallas_call(
        kernel,
        in_specs=specs,
        out_shape=out_shape if not hbm else pltpu.HBM(out_shape.shape, out_shape.dtype),
        out_specs=jax.tree.map(lambda _: pl.BlockSpec(memory_space=pltpu.VMEM), out_shape),
        scratch_shapes=list(scratch),
        interpret=INTERPRET,
        name=kernel.__name__,
        compiler_params=pltpu.CompilerParams(vmem_limit_bytes=48 * 1024 * 1024),
    )(*args)


def shape(*dims):
    return jax.ShapeDtypeStruct(dims, F32)


def ring(axis):
    count = lax.axis_size(axis)
    up = [(i, (i + 1) % count) for i in range(count)]
    return up, [(b, a) for a, b in up]


def edges(axis, first, last):
    up, down = ring(axis)
    return lax.ppermute(last, axis, up), lax.ppermute(first, axis, down)


def body(spectrum, scalar):
    wave_first = waves_np(N1).astype(np.float32)[None]
    wave_second = np.repeat(waves_np(N2).astype(np.float32), 2)[:, None]
    blocks = np.tile(waves_np(N3).astype(np.float32).reshape(GY, 1, Q3), (1, 16, 1)).reshape(GY, 1, 256)
    wave_third = lax.dynamic_index_in_dim(jnp.asarray(blocks), lax.axis_index("py"), 0, keepdims=False)
    first = [jnp.asarray(t) for t in first_table()]
    second = [jnp.asarray(t) for t in second_forward()]
    third = [jnp.asarray(t) for t in third_forward()]
    x_low, x_high = edges("px", scalar[:EDGE], scalar[-EDGE:])
    around = jnp.concatenate([x_low[2:], scalar, x_high[:4]], axis=0)
    strips = [
        jnp.concatenate([around[2 * n : 40 - 2 * n, at : at + 2] for n, at in enumerate(starts)], axis=0)
        for starts in ((0, 2, 4), (2 * C2 - 2, 2 * C2 - 4, 2 * C2 - 6))
    ]
    y_low, y_high = edges("py", *strips)
    part = jnp.asarray(parity_table())
    brick = call(
        brick_kernel, shape(SLABS, 2, ROWS, 128), scalar, x_low, x_high, y_low, y_high, part,
        scratch=(pltpu.VMEM((SLABS, ROWS, 256), F32),),
    )
    sent = call(
        first_kernel, shape(GX, 80, 128), spectrum, jnp.asarray(wave_first), *first,
        scratch=(pltpu.VMEM((5 * N1, 128), F32),),
    )
    got = lax.all_to_all(sent, "px", split_axis=0, concat_axis=0, tiled=True)
    sent = call(second_kernel, shape(GY, 384, 128), got, jnp.asarray(wave_second), wave_third, *second, x_low, x_high, late=2, hbm=True)
    got = lax.all_to_all(sent, "py", split_axis=0, concat_axis=0, tiled=True)
    velocity, vorticity = call(
        third_kernel, (shape(3, C1, C2, N3), shape(3, C1, C2, N3)), got, *third
    )
    vx_low, vx_high = edges("px", velocity[:, :4], velocity[:, -4:])
    strips = [
        jnp.concatenate([part[:, :, cut] for part in (vx_low, velocity, vx_high)], axis=1)
        for cut in (slice(0, 4), slice(C2 - 4, C2))
    ]
    vy_low, vy_high = edges("py", *strips)
    theta, sent = call(
        scalar_kernel, (shape(2 * C1, 2 * C2, 2 * N3), shape(GY, 192, 128)),
        brick, velocity, vx_low, vx_high, vy_low, vy_high, vorticity,
        jnp.asarray(rise_tables()), part, *third,
        scratch=(
            pltpu.VMEM((SLABS, 2, ROWS, 128), F32),
            pltpu.VMEM((SLABS, 2, ROWS, 128), F32),
            pltpu.VMEM((2 * C1, 2 * C2, 256), F32),
            pltpu.VMEM((3 * PTS, PROWS, N3), F32),
            pltpu.VMEM((2 * 3 * PTS * PROWS, 128), F32),
            pltpu.VMEM((2 * 3 * PTS * ROWS, 128), F32),
            pltpu.VMEM((SLABS, 2, ROWS, 128), F32),
            pltpu.VMEM((SLABS, 2, ROWS, 128), F32),
            pltpu.VMEM((SLABS, 3, ROWS, 128), F32),
            pltpu.VMEM((2 * C1 * C2, 128), F32),
        ),
    )
    got = lax.all_to_all(sent, "py", split_axis=0, concat_axis=0, tiled=True)
    sent = call(
        second_back_kernel, shape(GX, 48, 128), got, *second
    )
    got = lax.all_to_all(sent, "px", split_axis=0, concat_axis=0, tiled=True)
    tendency = call(
        first_back_kernel, shape(2, 3, Q2, Q3, N1), got, *first,
        scratch=(pltpu.VMEM((N1, 128), F32),),
    )
    return tendency, theta


def solution(mesh):
    in_specs = (P(None, None, "px", "py", None), P("px", "py", None))
    out_specs = (P(None, None, "px", "py", None), P("px", "py", None))
    return jax.shard_map(body, mesh=mesh, in_specs=in_specs, out_specs=out_specs, check_vma=False)
```

```python
import math

import jax
import jax.numpy as jnp
import numpy as np
from jax import lax
from jax.experimental import pallas as pl
from jax.experimental.pallas import tpu as pltpu
from jax.sharding import PartitionSpec as P


NSUB = 3
STEP_RATIO = 0.08
DIFFUSION_RATIO = 1.0
INTERPRET = False

N1, N2, N3 = 512, 128, 128
GX, GY = 32, 8
Q2, Q3 = N2 // GX, N3 // GY
C1, C2 = N1 // GX, N2 // GY
FACTOR = 1.0 / math.sqrt(N1 * N2 * N3)
BF = jnp.bfloat16
F32 = jnp.float32


def halves(table):
    high = table.astype(np.float32).astype(BF)
    low = (table - high.astype(np.float64)).astype(np.float32).astype(BF)
    return np.asarray(high), np.asarray(low)


def waves_np(n):
    index = np.arange(n)
    return 2.0 * math.pi / n * np.where(index < n // 2, index, index - n)


def angles(n):
    index = np.arange(n)
    return 2.0 * math.pi / n * (np.outer(index, index) % n)


def first_table():
    a = angles(N1)[:, : N1 // 2]
    rows = np.concatenate([a[0::2], a[1::2]], axis=0)
    return halves(np.concatenate([np.cos(rows), np.sin(rows)], axis=1))


def second_forward():
    a = angles(N2)
    table = np.zeros((2, N2, N2, 2))
    table[0, :, :, 0] = np.cos(a)
    table[0, :, :, 1] = -np.sin(a)
    table[1, :, :, 0] = np.sin(a)
    table[1, :, :, 1] = np.cos(a)
    return halves(table.reshape(2 * N2, 2 * N2))


def third_forward():
    a = angles(N3)
    return halves(FACTOR * np.concatenate([np.cos(a), -np.sin(a)], axis=0))


def split(x):
    high = x.astype(BF)
    return high, (x - high.astype(F32)).astype(BF)


def dots(pairs, dims):
    total = None
    for left, right in pairs:
        part = lax.dot_general(left, right, (dims, ((), ())), preferred_element_type=F32)
        total = part if total is None else total + part
    return total


def dot3(left, right, dims=((1,), (0,))):
    lh, ll = left
    rh, rl = right
    return dots([(lh, rl), (ll, rh), (lh, rh)], dims)


def swap_groups(v):
    lane = lax.broadcasted_iota(jnp.int32, v[0].shape, len(v[0].shape) - 1) // 16
    axis = len(v[0].shape) - 1
    v = list(v)
    for s in (1, 2, 4):
        upper = (lane // s) % 2 == 1
        for i in range(8):
            if i & s:
                continue
            a, b = v[i], v[i + s]
            v[i] = jnp.where(upper, pltpu.roll(b, 16 * s, axis), a)
            v[i + s] = jnp.where(upper, b, pltpu.roll(a, 128 - 16 * s, axis))
    return v


HALF = N1 // 2


def point_row(i):
    return HALF * (i % 2) + i // 2


def first_kernel(spec_far, wave_far, th_far, tl_far, out, y, spec, wave, th, tl, landed):
    far, near = (spec_far, wave_far, th_far, tl_far), (spec, wave, th, tl)
    copies = [pltpu.make_async_copy(a, b, landed.at[n]) for n, (a, b) in enumerate(zip(far, near))]
    for copy in copies:
        copy.start()
    for copy in copies:
        copy.wait()
    even, odd = [], []
    for n, f in enumerate((0, 1, 2, 1, 2)):
        plain, turned = [], []
        for r in range(Q2):
            re, im = spec[0, f, r], spec[1, f, r]
            if n > 2:
                re, im = re * wave[...], im * wave[...]
            plain += [re, im]
            turned += [-im, re]
        pieces = [jnp.concatenate(part, axis=0) for part in (plain, turned)]
        even.append(jnp.concatenate([p[:, :HALF] + p[:, HALF:] for p in pieces], axis=1))
        odd.append(jnp.concatenate([p[:, :HALF] - p[:, HALF:] for p in pieces], axis=1))
    for n, rows in enumerate((even, odd)):
        table = (th[HALF * n : HALF * n + HALF, :], tl[HALF * n : HALF * n + HALF, :])
        z = dot3(table, split(jnp.concatenate(rows, axis=0)), ((1,), (1,)))
        for f in range(5):
            at = N1 * f + HALF * n
            y[at : at + HALF, :] = z[:, 128 * f : 128 * f + 128]
    for f in range(5):
        w = swap_groups([y[pl.ds(N1 * f + point_row(i), N1 // 8, stride=4), :] for i in range(8)])
        for g in range(8):
            y[pl.ds(N1 * f + g, N1 // 8, stride=8), :] = w[g]
        out[:, 16 * f : 16 * f + 16, :] = y[N1 * f : N1 * f + N1, :].reshape(GX, 16, 128)


def second_kernel(got, wave2, wave3, th, tl, x_low, x_high, out):
    c = []
    for f in range(5):
        halves_ = [got[:, 16 * f + 8 * h : 16 * f + 8 * h + 8, :].reshape(256, 128) for h in range(2)]
        c.append(jnp.concatenate(halves_, axis=1))
    k2 = wave2[...]
    k3 = wave3[...]
    curl = [k2 * c[2] - k3 * c[1], k3 * c[0] - c[4], c[3] - k2 * c[0]]
    z = dot3((th[...], tl[...]), split(jnp.concatenate(c[:3] + curl, axis=1)))
    for f in range(6):
        real = z[:128, 256 * f : 256 * f + 256]
        imag = z[128:, 256 * f : 256 * f + 256]
        for ri, part in enumerate((real, imag) if f < 3 else (-imag, real)):
            for h in range(2):
                at = ((f * 2 + ri) * 2 + h) * 16
                out[:, at : at + 16, :] = part[:, h * 128 : h * 128 + 128].reshape(GY, 16, 128)


def third_kernel(got, th, tl, velocity, vorticity):
    for f in range(6):
        lines = []
        for ri in range(2):
            blocks = []
            for h in range(2):
                at = ((f * 2 + ri) * 2 + h) * 16
                blocks += swap_groups([got[q, at : at + 16, :] for q in range(GY)])
            lines.append(jnp.concatenate(blocks, axis=0))
        u = dot3(split(jnp.concatenate(lines, axis=1)), (th[...], tl[...]))
        out = velocity if f < 3 else vorticity
        out[f % 3] = u.reshape(C1, C2, N3)


def force_lines(velocity, vorticity, b, th, tl, out):
    u = [velocity[i].reshape(C1 * C2, N3) for i in range(3)]
    w = [vorticity[i].reshape(C1 * C2, N3) for i in range(3)]
    force = [u[1] * w[2] - u[2] * w[1], u[2] * w[0] - u[0] * w[2], u[0] * w[1] - u[1] * w[0] + b]
    for f in range(3):
        lines = dot3(split(force[f]), (th[...], tl[...]), ((1,), (1,)))
        for ri in range(2):
            for h in range(2):
                at = ((f * 2 + ri) * 2 + h) * 16
                v = [
                    lines[(h * 8 + i) * 16 : (h * 8 + i) * 16 + 16, ri * 128 : ri * 128 + 128]
                    for i in range(8)
                ]
                w8 = swap_groups(v)
                for q in range(GY):
                    out[q, at : at + 16, :] = w8[q]


def parted(table):
    return np.concatenate([table[:, 0::2], table[:, 1::2]], axis=1).astype(np.float32).astype(BF)


def rise_tables():
    plain = np.zeros((N3, 2 * N3))
    for i in range(N3):
        plain[i, 2 * i] += 1.0
        for near in (i, (i + 1) % N3):
            plain[near, 2 * i + 1] += 9.0 / 16.0
        for far in ((i - 1) % N3, (i + 2) % N3):
            plain[far, 2 * i + 1] -= 1.0 / 16.0
    face = 0.5 * (plain + np.roll(plain, -1, axis=1))
    return np.stack([parted(plain), parted(face)])


def parity_table():
    return parted(np.eye(2 * N3))


def three(x):
    high, rest = x.astype(BF), None
    rest = x - high.astype(F32)
    mid = rest.astype(BF)
    return (rest - mid.astype(F32)).astype(BF), mid, high


def permuted(x, table, dims=((1,), (0,))):
    return dots([(part, table) for part in three(x)], dims)


def middle(a, b, c, d):
    return (9.0 * (b + c) - (a + d)) * (1.0 / 16.0)


def limited(first, second):
    return jnp.maximum(jnp.minimum(second, 0.0), jnp.minimum(first, jnp.maximum(second, 0.0)))


def upwind(face, left, right, jump):
    return face * jnp.where(face > 0.0, left, right) - DIFFUSION_RATIO * jump


def row_divergence(theta, face):
    count = theta.shape[0]
    jump = pltpu.roll(theta, count - 1, 0) - theta
    half = 0.5 * limited(pltpu.roll(jump, 1, 0), jump)
    flux = upwind(face, theta + half, pltpu.roll(theta - half, count - 1, 0), jump)
    return flux - pltpu.roll(flux, 1, 0)


def lane_divergence(even, odd, face_even, face_odd, face_before):
    even_before, odd_before = pltpu.roll(even, 1, 1), pltpu.roll(odd, 1, 1)
    even_after, odd_after = pltpu.roll(even, N3 - 1, 1), pltpu.roll(odd, N3 - 1, 1)
    jump_even = odd - even
    jump_odd = even_after - odd
    jump_before = even - odd_before
    half_even = 0.5 * limited(jump_before, jump_even)
    half_odd = 0.5 * limited(jump_even, jump_odd)
    half_before = 0.5 * limited(odd_before - even_before, jump_before)
    half_after = 0.5 * limited(jump_odd, odd_after - even_after)
    flux_even = upwind(face_even, even + half_even, odd - half_odd, jump_even)
    flux_odd = upwind(face_odd, odd + half_odd, even_after - half_after, jump_odd)
    flux_before = upwind(face_before, odd_before + half_before, even - half_even, jump_before)
    return flux_even - flux_before, flux_odd - flux_even


EDGE = 6
SLABS = 2 * C1 + 2 * EDGE
ROWS = 2 * C2 + 16
PTS = C1 + 8
PROWS = C2 + 16


def brick_kernel(scalar, x_low, x_high, y_low, y_high, table, brick, raw):
    raw[0:EDGE, 8:40, :] = x_low[...]
    raw[EDGE : EDGE + 2 * C1, 8:40, :] = scalar[...]
    raw[EDGE + 2 * C1 :, 8:40, :] = x_high[...]
    at = 0
    for layer in range(3):
        first, count = 2 + 2 * layer, 40 - 4 * layer
        raw[first : first + count, 6 - 2 * layer : 8 - 2 * layer, :] = y_low[at : at + count]
        raw[first : first + count, 40 + 2 * layer : 42 + 2 * layer, :] = y_high[at : at + count]
        at += count

    def sort(n, carry):
        z = permuted(raw[pl.ds(4 * n, 4)].reshape(4 * ROWS, 256), table[...])
        for h in range(2):
            brick[pl.ds(4 * n, 4), h] = z[:, h * 128 : h * 128 + 128].reshape(4, ROWS, 128)
        return carry

    lax.fori_loop(0, SLABS // 4, sort, 0)


def scalar_kernel(
    brick, velocity, vx_low, vx_high, vy_low, vy_high, vorticity,
    rise, part, th, tl,
    advanced, out,
    ta, tb, last, vw, su, sf, f1, f2, f3, bs,
):
    for c in range(3):
        vw[c * PTS : c * PTS + 4, 8:24, :] = vx_low[c]
        vw[c * PTS + 4 : c * PTS + 20, 8:24, :] = velocity[c]
        vw[c * PTS + 20 : c * PTS + 24, 8:24, :] = vx_high[c]
        vw[c * PTS : c * PTS + 24, 4:8, :] = vy_low[c]
        vw[c * PTS : c * PTS + 24, 24:28, :] = vy_high[c]
    total = 3 * PTS * PROWS
    for c in range(3):
        table = rise[1 if c == 2 else 0]

        def third(n, carry, c=c, table=table):
            lines = vw[pl.ds(c * PTS + 8 * n, 8)].reshape(8 * PROWS, N3)
            high, low = split(lines)
            z = dots([(low, table), (high, table)], ((1,), (0,)))
            at = pl.multiple_of((c * PTS + 8 * n) * PROWS, 8)
            for h in range(2):
                su[pl.ds(h * total + at, 8 * PROWS), :] = z[:, h * 128 : h * 128 + 128]
            return carry

        lax.fori_loop(0, PTS // 8, third, 0)

    def second(n, carry, c):
        for h in range(2):
            at = pl.multiple_of(h * total + (c * PTS + n) * PROWS, 8)
            p = su[pl.ds(at, PROWS), :]
            a, b, cc, d = (p[4 + o : 25 + o] for o in range(4))
            odd, even = middle(a, b, cc, d), cc
            to = (h * 3 * PTS + c * PTS + n) * ROWS
            if c == 1:
                sf[pl.ds(to + 3, 21, stride=2), :] = 0.5 * (odd + even)
                sf[pl.ds(to + 2, 21, stride=2), :] = 0.5 * (b + odd)
            else:
                sf[pl.ds(to + 3, 21, stride=2), :] = odd
                sf[pl.ds(to + 4, 21, stride=2), :] = even
        return carry

    for c in range(3):
        lax.fori_loop(0, PTS, lambda n, k, c=c: second(n, k, c), 0)

    def first(k, carry):
        for c, face in enumerate((f1, f2, f3)):
            for h in range(2):
                a, b, cc, d = (
                    sf[pl.ds(pl.multiple_of((h * 3 * PTS + c * PTS + k + o) * ROWS, 8), ROWS), :]
                    for o in range(4)
                )
                odd = middle(a, b, cc, d)
                if c == 0:
                    face[2 * k + 1, h] = 0.5 * (odd + cc)
                    face[2 * k, h] = 0.5 * (b + odd)
                else:
                    face[2 * k + 1, h] = odd
                    face[2 * k + 2, h] = cc
                if c == 2 and h == 1:
                    face[2 * k + 1, 2] = pltpu.roll(odd, 1, 1)
                    face[2 * k + 2, 2] = pltpu.roll(cc, 1, 1)
        return carry

    lax.fori_loop(0, 21, first, 0)

    for turn, (source, target) in enumerate(((brick, ta), (ta, tb), (tb, last))):
        low = 2 + 2 * turn
        begin = []
        for h in range(2):
            t0, t1, t2, t3 = (source[low - 2 + o, h] for o in range(4))
            j0, j1, j2 = t1 - t0, t2 - t1, t3 - t2
            h1, h2 = 0.5 * limited(j0, j1), 0.5 * limited(j1, j2)
            begin.append((t2 + h2, j2, upwind(f1[low - 1, h], t1 + h1, t2 - h2, j1)))

        def step(i, carry, source=source, target=target, turn=turn):
            here = [source[i, h] for h in range(2)]
            change = list(lane_divergence(*here, f3[i, 0], f3[i, 1], f3[i, 2]))
            done = []
            for h in range(2):
                left, jump, before = carry[h]
                ahead = source[i + 1, h]
                next_jump = source[i + 2, h] - ahead
                half = 0.5 * limited(jump, next_jump)
                flux = upwind(f1[i, h], left, ahead - half, jump)
                total = change[h] + (flux - before) + row_divergence(here[h], f2[i, h])
                fresh = here[h] - STEP_RATIO * total
                if turn < NSUB - 1:
                    target[i, h] = fresh
                else:
                    target[i - EDGE, :, h * 128 : h * 128 + 128] = fresh[8:40]
                done.append((ahead + half, next_jump, flux))
            return tuple(done)

        lax.fori_loop(low, SLABS - low, step, tuple(begin))

    def finish(n, carry):
        lines = last[pl.ds(4 * n, 4)]
        advanced[pl.ds(4 * n, 4)] = permuted(lines.reshape(128, 256), part[...], ((1,), (1,))).reshape(4, 32, 256)
        both = lines[:, :, :128] + lines[:, :, 128:]
        bs[pl.ds(pl.multiple_of(64 * n, 8), 32), :] = 0.125 * (both[0] + both[1])
        bs[pl.ds(pl.multiple_of(64 * n + 32, 8), 32), :] = 0.125 * (both[2] + both[3])
        return carry

    lax.fori_loop(0, C1 // 2, finish, 0)
    buoyancy = bs[pl.ds(0, C1 * C2, stride=2), :] + bs[pl.ds(1, C1 * C2, stride=2), :]
    force_lines(velocity, vorticity, buoyancy, th, tl, out)


def second_back_kernel(got, th, tl, out):
    columns = []
    for f in range(3):
        for h in range(2):
            parts = []
            for ri in range(2):
                at = ((f * 2 + ri) * 2 + h) * 16
                parts.append(got[:, at : at + 16, :].reshape(128, 128))
            columns.append(jnp.concatenate(parts, axis=0))
    z = dot3((th[...], tl[...]), split(jnp.concatenate(columns, axis=1)), ((0,), (0,)))
    for f in range(3):
        for h in range(2):
            at = f * 16 + h * 8
            col = (f * 2 + h) * 128
            out[:, at : at + 8, :] = z[:, col : col + 128].reshape(GX, 8, 128)


def first_back_kernel(got, th, tl, out, y):
    rows = ([], [])
    for f in range(3):
        y[...] = got[:, 16 * f : 16 * f + 16, :].reshape(N1, 128)
        w = swap_groups([y[pl.ds(g, N1 // 8, stride=8), :] for g in range(8)])
        for i in range(8):
            y[pl.ds(point_row(i), N1 // 8, stride=4), :] = w[i]
        for n in range(2):
            rows[n].append(y[HALF * n : HALF * n + HALF, :].T)
    z = []
    for n in range(2):
        table = (th[HALF * n : HALF * n + HALF, :], tl[HALF * n : HALF * n + HALF, :])
        z.append(dot3(split(jnp.concatenate(rows[n], axis=0)), table))
    for f in range(3):
        for r in range(Q2):
            at = f * 128 + r * 32
            real = [p[at : at + 16, :HALF] + p[at + 16 : at + 32, HALF:] for p in z]
            imag = [p[at + 16 : at + 32, :HALF] - p[at : at + 16, HALF:] for p in z]
            for ri, (e, o) in enumerate((real, imag)):
                out[ri, f, r] = jnp.concatenate([e + o, e - o], axis=1)


def call(kernel, out_shape, *args, scratch=(), late=0, hbm=False, far=False):
    if far:
        args = [pltpu.with_memory_space_constraint(a, pltpu.HBM) for a in args]
    specs = [pl.BlockSpec(memory_space=pltpu.HBM if far else pltpu.VMEM)] * (len(args) - late)
    specs += [pl.BlockSpec(memory_space=pl.ANY)] * late
    return pl.pallas_call(
        kernel,
        in_specs=specs,
        out_shape=out_shape if not hbm else pltpu.HBM(out_shape.shape, out_shape.dtype),
        out_specs=jax.tree.map(lambda _: pl.BlockSpec(memory_space=pltpu.VMEM), out_shape),
        scratch_shapes=list(scratch),
        interpret=INTERPRET,
        compiler_params=pltpu.CompilerParams(vmem_limit_bytes=48 * 1024 * 1024),
    )(*args)


def shape(*dims):
    return jax.ShapeDtypeStruct(dims, F32)


def ring(axis):
    count = lax.axis_size(axis)
    up = [(i, (i + 1) % count) for i in range(count)]
    return up, [(b, a) for a, b in up]


def edges(axis, first, last):
    up, down = ring(axis)
    low = lax.ppermute(last, axis, up)
    return low, lax.ppermute(first, axis, down)


def step(spectrum, scalar):
    wave_first = waves_np(N1).astype(np.float32)[None]
    wave_second = np.repeat(waves_np(N2).astype(np.float32), 2)[:, None]
    blocks = np.tile(waves_np(N3).astype(np.float32).reshape(GY, 1, Q3), (1, 16, 1)).reshape(GY, 1, 256)
    wave_third = lax.dynamic_index_in_dim(jnp.asarray(blocks), lax.axis_index("py"), 0, keepdims=False)
    first = [jnp.asarray(t) for t in first_table()]
    second = [jnp.asarray(t) for t in second_forward()]
    third = [jnp.asarray(t) for t in third_forward()]
    x_low, x_high = edges("px", scalar[:EDGE], scalar[-EDGE:])
    around = jnp.concatenate([x_low[2:], scalar, x_high[:4]], axis=0)
    strips = [
        jnp.concatenate([around[2 * n : 40 - 2 * n, at : at + 2] for n, at in enumerate(starts)], axis=0)
        for starts in ((0, 2, 4), (2 * C2 - 2, 2 * C2 - 4, 2 * C2 - 6))
    ]
    y_low, y_high = edges("py", *strips)
    part = jnp.asarray(parity_table())
    brick = call(
        brick_kernel, shape(SLABS, 2, ROWS, 128), scalar, x_low, x_high, y_low, y_high, part,
        scratch=(pltpu.VMEM((SLABS, ROWS, 256), F32),),
    )
    sent = call(
        first_kernel, shape(GX, 80, 128), spectrum, jnp.asarray(wave_first), *first,
        scratch=(
            pltpu.VMEM((5 * N1, 128), F32),
            pltpu.VMEM((2, 3, Q2, Q3, N1), F32),
            pltpu.VMEM((1, N1), F32),
            pltpu.VMEM((N1, N1), BF),
            pltpu.VMEM((N1, N1), BF),
            pltpu.SemaphoreType.DMA((4,)),
        ),
        far=True, hbm=True,
    )
    got = lax.all_to_all(sent, "px", split_axis=0, concat_axis=0, tiled=True)
    sent = call(second_kernel, shape(GY, 384, 128), got, jnp.asarray(wave_second), wave_third, *second, x_low, x_high, late=2, hbm=True)
    got = lax.all_to_all(sent, "py", split_axis=0, concat_axis=0, tiled=True)
    velocity, vorticity = call(
        third_kernel, (shape(3, C1, C2, N3), shape(3, C1, C2, N3)), got, *third
    )
    vx_low, vx_high = edges("px", velocity[:, :4], velocity[:, -4:])
    strips = [
        jnp.concatenate([part[:, :, cut] for part in (vx_low, velocity, vx_high)], axis=1)
        for cut in (slice(0, 4), slice(C2 - 4, C2))
    ]
    vy_low, vy_high = edges("py", *strips)
    theta, sent = call(
        scalar_kernel, (shape(2 * C1, 2 * C2, 2 * N3), shape(GY, 192, 128)),
        brick, velocity, vx_low, vx_high, vy_low, vy_high, vorticity,
        jnp.asarray(rise_tables()), part, *third,
        scratch=(
            pltpu.VMEM((SLABS, 2, ROWS, 128), F32),
            pltpu.VMEM((SLABS, 2, ROWS, 128), F32),
            pltpu.VMEM((2 * C1, 2 * C2, 256), F32),
            pltpu.VMEM((3 * PTS, PROWS, N3), F32),
            pltpu.VMEM((2 * 3 * PTS * PROWS, 128), F32),
            pltpu.VMEM((2 * 3 * PTS * ROWS, 128), F32),
            pltpu.VMEM((SLABS, 2, ROWS, 128), F32),
            pltpu.VMEM((SLABS, 2, ROWS, 128), F32),
            pltpu.VMEM((SLABS, 3, ROWS, 128), F32),
            pltpu.VMEM((2 * C1 * C2, 128), F32),
        ),
    )
    got = lax.all_to_all(sent, "py", split_axis=0, concat_axis=0, tiled=True)
    sent = call(
        second_back_kernel, shape(GX, 48, 128), got, *second
    )
    got = lax.all_to_all(sent, "px", split_axis=0, concat_axis=0, tiled=True)
    tendency = call(
        first_back_kernel, shape(2, 3, Q2, Q3, N1), got, *first,
        scratch=(pltpu.VMEM((N1, 128), F32),),
    )
    return tendency, theta


def solution(mesh):
    in_specs = (P(None, None, "px", "py", None), P("px", "py", None))
    out_specs = (P(None, None, "px", "py", None), P("px", "py", None))
    return jax.shard_map(step, mesh=mesh, in_specs=in_specs, out_specs=out_specs, check_vma=False)
```
